32 devices in a mesh: rows: 8 (over z, x), probe: 4 (over y, core).
Axes of the slice: x: 2, y: 2, z: 4, core: 2. Of those that a mesh axis runs over, the one named last changes fastest.
Arguments:
- start_block: float32 [8, 32768], P('probe', 'rows'), may hold values from -6 to 6
- blocks: bfloat16 [1024, 128, 128], P('rows'), may hold values from 0 to 3, as said below
- block_rows: int32 [1024], P('rows'), may hold values from 0 to 31
- block_cols: int32 [1024], P('rows'), may hold values from 0 to 63
- counts: int32 [8], P('rows'), may hold values from 32 to 128, as said below
- boundary: int32 [2, 16384], P(None, 'rows'), may hold values from 0 to 4095, as said below
Outputs:
- basis: float32 [8, 32768], P('probe', 'rows')
- alpha_blocks: float32 [3, 8, 8], replicated
- beta_blocks: float32 [3, 8, 8], replicated
The draws below stay inside these ranges and needn't reach their ends.
Inputs may be any that keep to these rules, and one draw needn't show every extreme that they name: `blocks`: nonnegative edge weights, most entries zero. `counts`: one or more partitions have all 128 slots live. `boundary`: the 2048 entries of one list for one partition are distinct rows of that partition.
All inputs are finite; a program needn't handle non-finite values.
Results may differ from the reference program's by a relative error of at most 0.00525.
Values may be sent and summed in bfloat16 or wider, within the bound.
A program may use at most 64 MiB of HBM per device.

```python
import jax
import jax.numpy as jnp
from jax import lax

PROBES = 8
BLOCK = 128
ROW_BLOCKS = 32
STEPS = 3
HALO = 2048
MAXB = 128
NODES = 32768
N_ROWS = 8


def draw_blocks(key, part):
    shape = (N_ROWS * MAXB, BLOCK, BLOCK)
    pick_key, value_key = jax.random.split(key)
    chance = jax.random.uniform(pick_key, shape, jnp.float32)
    weight = jnp.exp(jax.random.uniform(value_key, shape, jnp.float32, jnp.log(0.2), jnp.log(2.0)))
    return jnp.where(chance < 0.15, weight, 0.0).astype(jnp.bfloat16)


def draw_counts(key, part):
    first_key, second_key = jax.random.split(key)
    divisor = jax.random.randint(first_key, (N_ROWS,), 1, 5)
    live_slots = MAXB // divisor
    chosen = jax.random.randint(second_key, (), 0, N_ROWS)
    return jnp.where(jnp.arange(N_ROWS) == chosen, MAXB, live_slots).astype(jnp.int32)


def draw_boundary(key, part):
    keys_all = jax.random.split(key, 2 * N_ROWS)
    rows_dev = ROW_BLOCKS * BLOCK
    orders = jax.vmap(lambda one_key: jax.random.permutation(one_key, rows_dev))(keys_all)
    return orders[:, :HALO].reshape(2, N_ROWS * HALO).astype(jnp.int32)


def touch_ends(entries, own_key, smallest, top_value):
    longest = entries.shape.index(max(entries.shape))
    spots = []
    for shift in (0, 1):
        where = [jax.random.randint(jax.random.fold_in(own_key, axis), (), 0, length) for axis, length in enumerate(entries.shape)]
        where[longest] = (where[longest] + shift) % entries.shape[longest]
        spots.append(tuple(where))
    return entries.at[spots[0]].set(smallest).at[spots[1]].set(top_value)


def block_scale(rng, shape, pieces, low, high):
    factor_of = 1.0
    for position, parts in pieces:
        heights = jax.random.uniform(jax.random.fold_in(jax.random.fold_in(rng, 6), position), (parts,), jnp.float32, low / len(pieces), high / len(pieces))
        factor_of = factor_of * jnp.repeat(jnp.exp(heights), shape[position] // parts).reshape((-1,) + (1,) * (len(shape) - 1 - position))
    return factor_of


def normal_values(rng, dims, deviation, most, shards=(), held_as=jnp.bfloat16):
    array = deviation * jax.random.normal(rng, dims, jnp.float32)
    if shards:
        array = array * block_scale(rng, dims, shards, -0.22, 0.18)
    return jnp.clip(array, -most, most).astype(held_as)


def setup_inputs(seed: int = 0) -> dict:
    arg_keys = jax.random.split(jax.random.key(seed), 7)
    return {
        "start_block": normal_values(arg_keys[0], (PROBES, NODES), 1.0, 6.0, ((0, 4), (1, 8)), jnp.float32),
        "blocks": draw_blocks(jax.random.fold_in(arg_keys[6], 71), 0),
        "block_rows": touch_ends(jax.random.randint(arg_keys[2], (N_ROWS * MAXB,), 0, ROW_BLOCKS), jax.random.fold_in(arg_keys[2], 1), 0, ROW_BLOCKS - 1).astype(jnp.int32),
        "block_cols": touch_ends(jax.random.randint(arg_keys[3], (N_ROWS * MAXB,), 0, 2 * ROW_BLOCKS), jax.random.fold_in(arg_keys[3], 1), 0, (2 * ROW_BLOCKS) - 1).astype(jnp.int32),
        "counts": draw_counts(jax.random.fold_in(arg_keys[6], 71), 0),
        "boundary": draw_boundary(jax.random.fold_in(arg_keys[6], 71), 0),
    }


def apply_graph(scaled, blocks, block_rows, block_cols, counts, boundary):
    probe_count = scaled.shape[0]
    rows_dev = ROW_BLOCKS * BLOCK
    split_rows = scaled.reshape(probe_count, N_ROWS, rows_dev)
    bound = boundary.reshape(2, N_ROWS, HALO)
    from_lower = jnp.take_along_axis(jnp.roll(split_rows, 1, axis=1), jnp.roll(bound[1], 1, axis=0)[None], axis=2)
    from_upper = jnp.take_along_axis(jnp.roll(split_rows, -1, axis=1), jnp.roll(bound[0], -1, axis=0)[None], axis=2)
    extended = jnp.concatenate([split_rows, from_lower, from_upper], axis=2)
    extended = jnp.transpose(extended, (1, 0, 2))

    def partition(inputs):
        ext_part, tiles, tile_rows, tile_cols, live_count = inputs
        is_live = (jnp.arange(MAXB, dtype=jnp.int32) < live_count).astype(jnp.float32)
        tiles32 = tiles.astype(jnp.float32)
        columns = ext_part.reshape(probe_count, 2 * ROW_BLOCKS, BLOCK)
        x_cols = columns[:, tile_cols].astype(jnp.float32)
        x_rows = columns[:, :ROW_BLOCKS][:, tile_rows].astype(jnp.float32)
        forward = jnp.einsum('pkj,kij->pki', x_cols, tiles32) * is_live[None, :, None]
        backward = jnp.einsum('pki,kij->pkj', x_rows, tiles32) * is_live[None, :, None]
        row_sums = jnp.zeros((probe_count, ROW_BLOCKS, BLOCK), jnp.float32).at[:, tile_rows].add(forward)
        col_sums = jnp.zeros((probe_count, 2 * ROW_BLOCKS, BLOCK), jnp.float32).at[:, tile_cols].add(backward)
        summed = col_sums.reshape(probe_count, 2 * rows_dev)
        return summed.at[:, :rows_dev].add(row_sums.reshape(probe_count, rows_dev))
    summed = lax.map(partition, (extended, blocks.reshape(N_ROWS, MAXB, BLOCK, BLOCK), block_rows.reshape(N_ROWS, MAXB), block_cols.reshape(N_ROWS, MAXB), counts))
    own_part = summed[:, :, :rows_dev]
    lower_part = jnp.roll(summed[:, :, rows_dev:rows_dev + HALO], -1, axis=0)
    upper_part = jnp.roll(summed[:, :, rows_dev + HALO:], 1, axis=0)
    offsets = (jnp.arange(N_ROWS, dtype=jnp.int32) * rows_dev)[:, None]
    result = jnp.transpose(own_part, (1, 0, 2)).reshape(probe_count, NODES)
    result = result.at[:, (offsets + bound[1]).reshape(-1)].add(jnp.transpose(lower_part, (1, 0, 2)).reshape(probe_count, -1))
    result = result.at[:, (offsets + bound[0]).reshape(-1)].add(jnp.transpose(upper_part, (1, 0, 2)).reshape(probe_count, -1))
    return result

def gram_mean(left, right):
    return jnp.dot(left, right.T, precision=lax.Precision.HIGHEST) / NODES

def reference(start_block, blocks, block_rows, block_cols, counts, boundary):
    unit_rows = jnp.ones((1, NODES), jnp.bfloat16)
    degree = 1.0 + apply_graph(unit_rows, blocks, block_rows, block_cols, counts, boundary)[0]
    inv_root = 1.0 / jnp.sqrt(degree)

    def laplacian(vectors):
        scaled = (inv_root * vectors).astype(jnp.bfloat16)
        image = apply_graph(scaled, blocks, block_rows, block_cols, counts, boundary)
        return vectors - inv_root * (inv_root * vectors) - inv_root * image
    factor = jnp.linalg.cholesky(gram_mean(start_block, start_block))
    current = jax.scipy.linalg.solve_triangular(factor, start_block, lower=True)
    previous = jnp.zeros_like(current)
    coupling = jnp.zeros((PROBES, PROBES), jnp.float32)
    alpha_list = []
    beta_list = []
    for iteration in range(STEPS):
        image = laplacian(current)
        alpha_block = gram_mean(image, current)
        residual = image - jnp.dot(alpha_block, current, precision=lax.Precision.HIGHEST) - jnp.dot(coupling, previous, precision=lax.Precision.HIGHEST)
        factor = jnp.linalg.cholesky(gram_mean(residual, residual))
        previous = current
        current = jax.scipy.linalg.solve_triangular(factor, residual, lower=True)
        coupling = factor.T
        alpha_list.append(alpha_block)
        beta_list.append(factor)
    return (current, jnp.stack(alpha_list), jnp.stack(beta_list))
```

```python
import functools

import jax
import jax.numpy as jnp
from jax import lax
from jax.experimental import pallas as pl
from jax.experimental.pallas import tpu as pltpu
from jax.sharding import PartitionSpec as P

STEPS = 3
LANES = 128
PLANES = 2
RETURN_TYPE = jnp.float32
MESH = pl.DeviceIdType.MESH
BY_COL, COL_OTHER, COL_END, COL_KEEP, BY_ROW, ROW_OTHER, ROW_END, ROW_KEEP = range(8)


def kernel(
    n_rows, n_probe, node_total,
    start_ref, tiles_hbm, rows_ref, cols_ref, counts_ref, bound_ref,
    basis_ref, coef_ref,
    tiles, gathered, vec, scaled, inv_root, inverse, table_v, table,
    own, extended_0, extended_1, extended_2, halo_send, ret_send, ret_recv, deg_send, deg_recv, row_sums, col_sums, gram_send, gram_recv,
    tile_sem, table_sem, start_send, start_recv, halo_ssem, halo_rsem, ret_ssem, ret_rsem, deg_ssem, deg_rsem,
    gram_ssem, gram_rsem,
):
    me = lax.axis_index("rows")
    my_probe = lax.axis_index("probe")
    slots = tiles.shape[0]
    nb = inv_root.shape[0]
    nh = nb // 2
    probes_dev = start_ref.shape[0]
    lower = lax.rem(me + n_rows - 1, n_rows)
    upper = lax.rem(me + 1, n_rows)
    f32, bf16 = jnp.float32, jnp.bfloat16
    extended = (extended_0, extended_1, extended_2)

    tile_copy = pltpu.make_async_copy(tiles_hbm, tiles, tile_sem)
    tile_copy.start()

    barrier = pltpu.get_barrier_semaphore()
    for off in range(1, n_probe):
        peer = lax.rem(my_probe + off, n_probe)
        pl.semaphore_signal(barrier, inc=1, device_id={"probe": peer}, device_id_type=MESH)

    def greet(off, carry):
        peer = lax.rem(me + off, n_rows)
        pl.semaphore_signal(barrier, inc=1, device_id={"rows": peer}, device_id_type=MESH)
        return carry

    lax.fori_loop(1, n_rows, greet, 0)

    lane = lax.broadcasted_iota(jnp.int32, (8, LANES), 1)
    sub = lax.broadcasted_iota(jnp.int32, (8, LANES), 0)
    zero = jnp.zeros((8, LANES), f32)

    lane_s = lax.broadcasted_iota(jnp.int32, (slots, slots), 1).astype(f32)
    sub_s = lax.broadcasted_iota(jnp.int32, (slots, slots), 0).astype(f32)
    lane_k = lax.broadcasted_iota(jnp.int32, (slots, LANES), 1).astype(f32)
    diagonal = lane_s == sub_s
    slot = lax.broadcasted_iota(jnp.int32, (1, slots), 1)
    live = slot < counts_ref[0]

    def down(row):
        return jnp.sum(jnp.where(diagonal, jnp.broadcast_to(row, (slots, slots)), 0.0), axis=1, keepdims=True)

    def order(keys, other, others_most, first):
        key = jnp.where(live, keys, 2 * nb).astype(f32)
        key_down = down(key)
        other_down = down(other.astype(f32))
        key_row = jnp.broadcast_to(key, (slots, slots))
        same = key_row == key_down
        before = jnp.where(same, jnp.where(lane_s < sub_s, 1.0, 0.0), 0.0)
        rank = jnp.sum(jnp.where(key_row < key_down, 1.0, before), axis=1, keepdims=True)
        kept = jnp.where(jnp.sum(before, axis=1, keepdims=True) > 0.0, 1.0, 0.0)
        placed = rank == lane_s
        perm = jnp.sum(jnp.where(placed, sub_s, 0.0), axis=0, keepdims=True)
        others = jnp.sum(jnp.where(placed, other_down, 0.0), axis=0, keepdims=True)
        keep = jnp.sum(jnp.where(placed, kept, 0.0), axis=0, keepdims=True)
        up_to = jnp.sum(jnp.where(key_down <= lane_k, 1.0, 0.0), axis=0, keepdims=True)
        some = jnp.sum(jnp.where(key_down == lane_k, 1.0, 0.0), axis=0, keepdims=True)
        end = jnp.where(some > 0.0, up_to - 1.0, float(slots))
        rows = ((perm, slots - 1), (others, others_most), (end, slots), (keep, 1))
        for place, (value, most) in enumerate(rows):
            table_v[first + place : first + place + 1, :] = jnp.clip(value.astype(jnp.int32), 0, most)

    order(cols_ref[...], rows_ref[...], nb - 1, BY_COL)
    order(rows_ref[...], cols_ref[...], 2 * nb - 1, BY_ROW)
    table_copy = pltpu.make_async_copy(table_v, table, table_sem)
    table_copy.start()

    pl.semaphore_wait(barrier, n_probe - 1 + n_rows - 1)

    def start_copy(off):
        peer = lax.rem(my_probe + off, n_probe)
        return pltpu.make_async_remote_copy(
            src_ref=start_ref,
            dst_ref=gathered.at[my_probe],
            send_sem=start_send.at[off],
            recv_sem=start_recv.at[off],
            device_id={"probe": peer},
            device_id_type=MESH,
        )

    for off in range(1, n_probe):
        start_copy(off).start()
    gathered[my_probe] = start_ref[...]
    table_copy.wait()

    def row_of(k, block, probe):
        return jnp.broadcast_to(vec[k, pl.ds(block * 8 + probe, 1), :], (8, LANES))

    def block_of(k, block):
        return vec[k, pl.ds(pl.multiple_of(block * 8, 8), 8), :]

    def put_block(k, block, value):
        vec[k, pl.ds(pl.multiple_of(block * 8, 8), 8), :] = value

    def root_of(block):
        return jnp.broadcast_to(inv_root[pl.ds(block, 1), :], (8, LANES))

    def gram_copy(index, off):
        peer = lax.rem(me + off, n_rows)
        return pltpu.make_async_remote_copy(
            src_ref=gram_send.at[index],
            dst_ref=gram_recv.at[index, me],
            send_sem=gram_ssem.at[index, off],
            recv_sem=gram_rsem.at[index, off],
            device_id={"rows": peer},
            device_id_type=MESH,
        )

    def gram_begin(index, accs):
        gram = zero
        for q, acc in enumerate(accs):
            gram = jnp.where(lane == q, jnp.sum(acc, axis=1, keepdims=True), gram)
        gram_send[index] = gram
        gram_recv[index, me] = gram

        def send(off, carry):
            gram_copy(index, off).start()
            return carry

        lax.fori_loop(1, n_rows, send, 0)

    def gram_end(index, count):
        def wait(off, carry):
            gram_copy(index, off).wait()
            return carry

        lax.fori_loop(1, n_rows, wait, 0)
        gram = jnp.sum(gram_recv[index], axis=0) * (1.0 / node_total)
        return [jnp.broadcast_to(gram[:, q : q + 1], (8, LANES)) for q in range(count)]

    def grams(pairs):
        def body(block, accs):
            out = []
            for i, (left, right) in enumerate(pairs):
                value = block_of(left, block)
                out += [accs[i * 8 + q] + value * row_of(right, block, q) for q in range(8)]
            return tuple(out)

        return lax.fori_loop(0, nb, body, (zero,) * (8 * len(pairs)), unroll=8)

    def spread(column, row):
        return jnp.broadcast_to(column[row : row + 1, :], (8, LANES))

    def factorise(work):
        work = list(work)
        inverse_cols = [jnp.where(sub == q, 1.0, 0.0) for q in range(8)]
        factor = []
        scale = zero
        for j in range(8):
            root = lax.rsqrt(spread(work[j], j))
            scale = jnp.where(sub == j, root, scale)
            part = work[j] * root
            factor.append(jnp.where(sub >= j, part, 0.0))
            lower_part = jnp.where(sub > j, part * root, 0.0)
            for q in range(j + 1, 8):
                work[q] = work[q] - lower_part * spread(work[q], j)
            for q in range(j + 1):
                inverse_cols[q] = inverse_cols[q] - lower_part * spread(inverse_cols[q], j)
        inverse_cols = [column * scale for column in inverse_cols]
        transposed = [jnp.where(sub <= q, work[q] * scale, 0.0) for q in range(8)]
        return factor, inverse_cols, transposed

    def product(left, right):
        out = []
        for q in range(8):
            value = left[0] * spread(right[q], 0)
            for k in range(1, 8):
                value = value + left[k] * spread(right[q], k)
            out.append(value)
        return out

    def outer(left):
        out = []
        for q in range(8):
            value = left[0] * spread(left[0], q)
            for k in range(1, 8):
                value = value + left[k] * spread(left[k], q)
            out.append(value)
        return out

    def minus(left, right):
        return [a - b for a, b in zip(left, right)]

    def put_matrix(place, columns):
        value = zero
        for q in range(8):
            value = jnp.where(lane == q, columns[q], value)
        coef_ref[place] = value

    def mixed(terms, block):
        value = None
        for columns, k in terms:
            for q in range(8):
                part = columns[q] * row_of(k, block, q)
                value = part if value is None else value + part
        return value

    def mix(terms, target):
        def body(block, carry):
            put_block(target, block, mixed(terms, block))
            return carry

        lax.fori_loop(0, nb, body, 0, unroll=4)

    def folded(value):
        return value if value.shape[0] == 8 else value[:8] + value[8:]

    def col_products(lhs_of):
        def body(m, acc):
            y = jnp.dot(lhs_of(table[COL_OTHER, m]), tiles[table[BY_COL, m]], preferred_element_type=f32)
            acc = acc * table[COL_KEEP, m].astype(f32) + folded(y)
            col_sums[m] = acc
            return acc

        lax.fori_loop(0, slots, body, zero, unroll=64)

    def row_products(lhs_of):
        def body(m, acc):
            y = lax.dot_general(
                lhs_of(table[ROW_OTHER, m]), tiles[table[BY_ROW, m]], (((1,), (1,)), ((), ())),
                preferred_element_type=f32,
            )
            acc = acc * table[ROW_KEEP, m].astype(f32) + folded(y)
            row_sums[m] = acc
            return acc

        lax.fori_loop(0, slots, body, zero, unroll=64)

    row_sums[slots] = zero
    col_sums[slots] = zero

    def exchange(src, dst, ssem, rsem):
        return [
            pltpu.make_async_remote_copy(
                src_ref=src(side),
                dst_ref=dst(1 - side),
                send_sem=ssem(side),
                recv_sem=rsem(side),
                device_id={"rows": lower if side == 0 else upper},
                device_id_type=MESH,
            )
            for side in range(2)
        ]

    tile_copy.wait()
    ones = jnp.ones((8, LANES), bf16)
    col_products(lambda b: ones)
    for side in range(2):
        for c in range(nh):
            deg_send[side, c : c + 1, :] = col_sums[table[COL_END, nb + side * nh + c], 0:1, :]
    deg_copies = exchange(
        lambda side: deg_send.at[side], lambda side: deg_recv.at[side],
        lambda side: deg_ssem.at[side], lambda side: deg_rsem.at[side],
    )
    for copy in deg_copies:
        copy.start()

    for off in range(1, n_probe):
        start_copy(off).wait()

    def take_start(block, carry):
        where = pl.ds(pl.multiple_of(block * LANES, LANES), LANES)
        for g in range(n_probe):
            vec[0, pl.ds(block * 8 + g * probes_dev, probes_dev), :] = gathered[g, :, where]
        return carry

    lax.fori_loop(0, nb, take_start, 0, unroll=8)
    gram_begin(0, grams([(0, 0)]))

    row_products(lambda b: ones)

    sub_l = lax.broadcasted_iota(jnp.int32, (LANES, LANES), 0)
    sub_b = lax.broadcasted_iota(jnp.int32, (nb, LANES), 0)
    lane_b = lax.broadcasted_iota(jnp.int32, (nb, LANES), 1)
    for side in range(2):
        total = jnp.zeros((2 * nb, LANES), f32)
        for c in range(nh):
            where = bound_ref[side : side + 1, c * LANES : (c + 1) * LANES]
            in_block = sub_b == jnp.broadcast_to(jnp.right_shift(where, 7), (nb, LANES))
            at_lane = sub_l == jnp.broadcast_to(jnp.bitwise_and(where, LANES - 1), (LANES, LANES))
            h = lane_b + c * LANES
            high = jnp.where(in_block, (jnp.right_shift(h, 6) + 1).astype(f32), 0.0)
            low = jnp.where(in_block, jnp.bitwise_and(h, 63).astype(f32), 0.0)
            total = total + lax.dot_general(
                jnp.concatenate([high, low], axis=0).astype(bf16), jnp.where(at_lane, 1.0, 0.0).astype(bf16),
                (((1,), (1,)), ((), ())), preferred_element_type=f32,
            )
        inverse[pl.ds(side * nb, nb), :] = ((total[:nb] - 1.0) * 64.0 + total[nb:]).astype(jnp.int32)

    def found_of(source_of, where, count, kind):
        spot = jnp.bitwise_and(where, LANES - 1)
        block = jnp.right_shift(where, 7)
        found = zero
        for s in range(count):
            picked = jnp.take_along_axis(source_of(s).astype(f32), spot, axis=1, mode="promise_in_bounds")
            found = jnp.where(block == s, picked, found)
        return found

    for b in range(nb):
        inv_root[b : b + 1, :] = row_sums[table[ROW_END, b], 0:1, :] + col_sums[table[COL_END, b], 0:1, :]
    for copy in deg_copies:
        copy.wait()
    for g in range(nb // 8):
        degree = 1.0 + inv_root[g * 8 : g * 8 + 8, :]
        for side in range(2):
            degree = degree + found_of(
                lambda s: jnp.broadcast_to(deg_recv[side, s : s + 1, :], (8, LANES)),
                inverse[side * nb + g * 8 : side * nb + g * 8 + 8, :], nh, f32,
            )
        inv_root[g * 8 : g * 8 + 8, :] = 1.0 / jnp.sqrt(degree)

    def planes(value):
        top = value.astype(bf16)
        if PLANES == 1:
            return top
        return jnp.concatenate([top, (value - top.astype(f32)).astype(bf16)], axis=0)

    def scale_block(step, block, value):
        value = root_of(block) * value
        scaled[pl.ds(pl.multiple_of(block * 8, 8), 8), :] = value
        pieces = planes(value)
        own[block] = pieces
        extended[step][block] = pieces

    def send_halo(step):
        def gather_block(c, carry):
            for side in range(2):
                piece = bound_ref[side : side + 1, pl.ds(pl.multiple_of(c * LANES, LANES), LANES)]
                found = found_of(
                    lambda s: scaled[s * 8 : s * 8 + 8, :], jnp.broadcast_to(piece, (8, LANES)), nb, f32
                )
                halo_send[step, side, c] = planes(found)
            return carry

        lax.fori_loop(0, nh, gather_block, 0, unroll=2)
        copies = exchange(
            lambda side: halo_send.at[step, side], lambda side: extended[step].at[pl.ds(nb + side * nh, nh)],
            lambda side: halo_ssem.at[step, side], lambda side: halo_rsem.at[step, side],
        )
        for copy in copies:
            copy.start()
        return copies

    def send_returns(step):
        col_products(lambda b: own[b])
        for side in range(2):
            for c in range(nh):
                ret_send[step, side, c] = col_sums[table[COL_END, nb + side * nh + c]].astype(RETURN_TYPE)
        copies = exchange(
            lambda side: ret_send.at[step, side], lambda side: ret_recv.at[step, side],
            lambda side: ret_ssem.at[step, side], lambda side: ret_rsem.at[step, side],
        )
        for copy in copies:
            copy.start()
        return copies

    def combine(step, source, target):
        def body(block, carry):
            total = row_sums[table[ROW_END, block]] + col_sums[table[COL_END, block]]
            for side in range(2):
                where = jnp.broadcast_to(inverse[pl.ds(side * nb + block, 1), :], (8, LANES))
                total = total + found_of(lambda s: ret_recv[step, side, s], where, nh, f32)
            root = root_of(block)
            put_block(target, block, -(root * (root * block_of(source, block) + total)))
            return carry

        lax.fori_loop(0, nb, body, 0, unroll=4)

    start_at, image_at = 0, STEPS + 4

    def q_at(j):
        return j

    def u_at(j):
        return STEPS + j

    coupling = None
    for step in range(STEPS):
        source = start_at if step == 0 else u_at(step)

        if step == 0:
            def body(block, carry):
                scale_block(0, block, block_of(start_at, block))
                return carry

            lax.fori_loop(0, nb, body, 0, unroll=4)
        halos = send_halo(step)
        returns = send_returns(step)
        if step:
            mix(q_terms, q_at(step))
            gram_begin(step, grams([(u_at(step), u_at(step)), (u_at(step), q_at(step))]))
        for copy in halos:
            copy.wait()
        row_products(lambda b: extended[step][b])

        if step == 0:
            factor, inv_cols, next_coupling = factorise(gram_end(0, 8))
            q_terms = [(inv_cols, start_at)]
            u_terms = [(inv_cols, image_at)]
        else:
            gram = gram_end(step, 16)
            shift = gram[8:]
            rest = minus(gram[:8], outer(shift))
            if step > 1:
                rest = minus(rest, outer(coupling))
            factor, inv_cols, next_coupling = factorise(rest)
            put_matrix(step - 1, [column + jnp.where(sub == q, 1.0, 0.0) for q, column in enumerate(shift)])
            put_matrix(STEPS + step - 1, factor)
            less = [-column for column in product(inv_cols, shift)]
            q_terms = [(inv_cols, u_at(step)), (less, q_at(step))]
            u_terms = [(inv_cols, image_at), (less, u_at(step))]
            if step > 1:
                less = [-column for column in product(inv_cols, coupling)]
                q_terms.append((less, q_at(step - 1)))
                u_terms.append((less, u_at(step - 1)))
        coupling = next_coupling

        for copy in returns:
            copy.wait()
        combine(step, source, image_at)

        def next_image(block, carry):
            value = mixed(u_terms, block)
            put_block(u_at(step + 1), block, value)
            if step + 1 < STEPS:
                scale_block(step + 1, block, value)
            return carry

        lax.fori_loop(0, nb, next_image, 0, unroll=4)

    mix(q_terms, q_at(STEPS))
    gram_begin(STEPS, grams([(u_at(STEPS), u_at(STEPS)), (u_at(STEPS), q_at(STEPS))]))
    gram = gram_end(STEPS, 16)
    shift = gram[8:]
    rest = minus(minus(gram[:8], outer(shift)), outer(coupling))
    factor, inv_cols, _ = factorise(rest)
    put_matrix(STEPS - 1, [column + jnp.where(sub == q, 1.0, 0.0) for q, column in enumerate(shift)])
    put_matrix(2 * STEPS - 1, factor)
    q_terms = [
        (inv_cols, u_at(STEPS)),
        ([-column for column in product(inv_cols, shift)], q_at(STEPS)),
        ([-column for column in product(inv_cols, coupling)], q_at(STEPS - 1)),
    ]
    mix(q_terms, start_at)
    for p in range(probes_dev):
        for b in range(nb):
            basis_ref[p : p + 1, b * LANES : (b + 1) * LANES] = vec[
                start_at, pl.ds(b * 8 + my_probe * probes_dev + p, 1), :
            ]


def local(start_block, blocks, block_rows, block_cols, counts, boundary):
    n_rows, n_probe = lax.axis_size("rows"), lax.axis_size("probe")
    probes_dev, rows_dev = start_block.shape
    slots = blocks.shape[0]
    nb = rows_dev // LANES
    nh = nb // 2
    f32, bf16 = jnp.float32, jnp.bfloat16
    vmem = pl.BlockSpec(memory_space=pltpu.VMEM)
    smem = pl.BlockSpec(memory_space=pltpu.SMEM)
    dma = pltpu.SemaphoreType.DMA
    height = 8 * PLANES
    basis, coef = pl.pallas_call(
        functools.partial(kernel, n_rows, n_probe, rows_dev * n_rows),
        out_shape=(
            jax.ShapeDtypeStruct((probes_dev, rows_dev), f32),
            jax.ShapeDtypeStruct((2 * STEPS, 8, LANES), f32),
        ),
        in_specs=[vmem, pl.BlockSpec(memory_space=pltpu.HBM), vmem, vmem, smem, vmem],
        out_specs=(vmem, vmem),
        scratch_shapes=[
            pltpu.VMEM(blocks.shape, bf16),
            pltpu.VMEM((n_probe, probes_dev, rows_dev), f32),
            pltpu.VMEM((2 * STEPS + 2, nb * 8, LANES), f32),
            pltpu.VMEM((nb * 8, LANES), f32),
            pltpu.VMEM((nb, LANES), f32),
            pltpu.VMEM((2 * nb, LANES), jnp.int32),
            pltpu.VMEM((8, LANES), jnp.int32),
            pltpu.SMEM((8, LANES), jnp.int32),
            pltpu.VMEM((nb, height, LANES), bf16),
            *[pltpu.VMEM((2 * nb, height, LANES), bf16)] * STEPS,
            pltpu.VMEM((STEPS, 2, nh, height, LANES), bf16),
            pltpu.VMEM((STEPS, 2, nh, 8, LANES), RETURN_TYPE),
            pltpu.VMEM((STEPS, 2, nh, 8, LANES), RETURN_TYPE),
            pltpu.VMEM((2, nh, LANES), f32),
            pltpu.VMEM((2, nh, LANES), f32),
            pltpu.VMEM((slots + 1, 8, LANES), f32),
            pltpu.VMEM((slots + 1, 8, LANES), f32),
            pltpu.VMEM((STEPS + 1, 8, LANES), f32),
            pltpu.VMEM((STEPS + 1, n_rows, 8, LANES), f32),
            dma,
            dma,
            dma((n_probe,)),
            dma((n_probe,)),
            dma((STEPS, 2)),
            dma((STEPS, 2)),
            dma((STEPS, 2)),
            dma((STEPS, 2)),
            dma((2,)),
            dma((2,)),
            dma((STEPS + 1, n_rows)),
            dma((STEPS + 1, n_rows)),
        ],
        compiler_params=pltpu.CompilerParams(
            collective_id=0, has_side_effects=True, vmem_limit_bytes=48 * 1024 * 1024
        ),
        name="lanczos",
    )(
        start_block, blocks, block_rows.reshape(1, slots), block_cols.reshape(1, slots), counts, boundary,
    )
    return basis, coef[:STEPS, :, :8], coef[STEPS:, :, :8]


def solution(mesh):
    in_specs = (
        P("probe", "rows"),
        P("rows", None, None),
        P("rows"),
        P("rows"),
        P("rows"),
        P(None, "rows"),
    )
    out_specs = (P("probe", "rows"), P(), P())
    return jax.shard_map(local, mesh=mesh, in_specs=in_specs, out_specs=out_specs, check_vma=False)
```

```python
import functools

import jax
import jax.numpy as jnp
from jax import lax
from jax.experimental import pallas as pl
from jax.experimental.pallas import tpu as pltpu
from jax.sharding import PartitionSpec as P

STEPS = 3
LANES = 128
PLANES = 2
PIECES = 4
VMEM_BYTES = 48 * 1024 * 1024
RETURN_TYPE = jnp.float32
MESH = pl.DeviceIdType.MESH
BY_COL, COL_OTHER, COL_END, COL_KEEP, BY_ROW, ROW_OTHER, ROW_END, ROW_KEEP = range(8)


def kernel(
    n_rows, n_probe, node_total,
    start_hbm, tiles_hbm, rows_hbm, cols_hbm, counts_hbm, bound_hbm,
    basis_ref, coef_ref,
    start_ref, tiles, turned, rows_ref, cols_ref, counts_ref, bound_ref, gathered, vec, scaled, inv_root, inverse, table_v, table,
    own, extended_0, extended_1, extended_2, halo_send, ret_send, ret_recv, deg_send, deg_recv, part_send, part_recv, row_sums, col_sums, gram_send, gram_recv,
    load_sem, table_sem, start_send, start_recv, halo_ssem, halo_rsem, ret_ssem, ret_rsem, part_ssem, part_rsem, deg_ssem, deg_rsem,
    gram_ssem, gram_rsem,
):
    me = lax.axis_index("rows")
    my_probe = lax.axis_index("probe")
    slots = tiles.shape[0]
    nb = inv_root.shape[0]
    nh = nb // 2
    probes_dev = start_ref.shape[0]
    lower = lax.rem(me + n_rows - 1, n_rows)
    upper = lax.rem(me + 1, n_rows)
    half = lax.rem(my_probe, 2)
    sibling = my_probe + 1 - 2 * half
    served = 1 - lax.rem(me + half, 2)
    partner = lax.rem(me + 2 * served - 1 + n_rows, n_rows)
    f32, bf16 = jnp.float32, jnp.bfloat16
    extended = (extended_0, extended_1, extended_2)

    loads = [
        pltpu.make_async_copy(source, target, load_sem.at[i])
        for i, (source, target) in enumerate(
            (
                (rows_hbm, rows_ref), (cols_hbm, cols_ref), (counts_hbm, counts_ref), (start_hbm, start_ref),
                (bound_hbm, bound_ref), (tiles_hbm, tiles),
            )
        )
    ]
    for load in loads:
        load.start()

    barrier = pltpu.get_barrier_semaphore()
    for off in range(1, n_probe):
        peer = lax.rem(my_probe + off, n_probe)
        pl.semaphore_signal(barrier, inc=1, device_id={"probe": peer}, device_id_type=MESH)

    def greet(off, carry):
        peer = lax.rem(me + off, n_rows)
        pl.semaphore_signal(barrier, inc=1, device_id={"rows": peer}, device_id_type=MESH)
        return carry

    lax.fori_loop(1, n_rows, greet, 0)

    lane = lax.broadcasted_iota(jnp.int32, (8, LANES), 1)
    sub = lax.broadcasted_iota(jnp.int32, (8, LANES), 0)
    zero = jnp.zeros((8, LANES), f32)

    lane_s = lax.broadcasted_iota(jnp.int32, (slots, slots), 1).astype(f32)
    sub_s = lax.broadcasted_iota(jnp.int32, (slots, slots), 0).astype(f32)
    lane_k = lax.broadcasted_iota(jnp.int32, (slots, LANES), 1).astype(f32)
    diagonal = lane_s == sub_s
    slot = lax.broadcasted_iota(jnp.int32, (1, slots), 1)
    for load in loads[:3]:
        load.wait()
    live = slot < counts_ref[0]

    def down(row):
        return jnp.sum(jnp.where(diagonal, jnp.broadcast_to(row, (slots, slots)), 0.0), axis=1, keepdims=True)

    def order(keys, other, others_most, first):
        key = jnp.where(live, keys, 2 * nb).astype(f32)
        key_down = down(key)
        other_down = down(other.astype(f32))
        key_row = jnp.broadcast_to(key, (slots, slots))
        same = key_row == key_down
        before = jnp.where(same, jnp.where(lane_s < sub_s, 1.0, 0.0), 0.0)
        rank = jnp.sum(jnp.where(key_row < key_down, 1.0, before), axis=1, keepdims=True)
        kept = jnp.where(jnp.sum(before, axis=1, keepdims=True) > 0.0, 1.0, 0.0)
        placed = rank == lane_s
        perm = jnp.sum(jnp.where(placed, sub_s, 0.0), axis=0, keepdims=True)
        others = jnp.sum(jnp.where(placed, other_down, 0.0), axis=0, keepdims=True)
        keep = jnp.sum(jnp.where(placed, kept, 0.0), axis=0, keepdims=True)
        up_to = jnp.sum(jnp.where(key_down <= lane_k, 1.0, 0.0), axis=0, keepdims=True)
        some = jnp.sum(jnp.where(key_down == lane_k, 1.0, 0.0), axis=0, keepdims=True)
        end = jnp.where(some > 0.0, up_to - 1.0, float(slots))
        rows = ((perm, slots - 1), (others, others_most), (end, slots), (keep, 1))
        for place, (value, most) in enumerate(rows):
            table_v[first + place : first + place + 1, :] = jnp.clip(value.astype(jnp.int32), 0, most)

    order(cols_ref[...], rows_ref[...], nb - 1, BY_COL)
    order(rows_ref[...], cols_ref[...], 2 * nb - 1, BY_ROW)
    table_copy = pltpu.make_async_copy(table_v, table, table_sem)
    table_copy.start()

    pl.semaphore_wait(barrier, n_probe - 1 + n_rows - 1)

    def start_copy(off):
        peer = lax.rem(my_probe + off, n_probe)
        return pltpu.make_async_remote_copy(
            src_ref=start_ref,
            dst_ref=gathered.at[my_probe],
            send_sem=start_send.at[off],
            recv_sem=start_recv.at[off],
            device_id={"probe": peer},
            device_id_type=MESH,
        )

    loads[3].wait()
    for off in range(1, n_probe):
        start_copy(off).start()
    gathered[my_probe] = start_ref[...]
    table_copy.wait()

    def row_of(k, block, probe):
        return jnp.broadcast_to(vec[k, pl.ds(block * 8 + probe, 1), :], (8, LANES))

    def block_of(k, block):
        return vec[k, pl.ds(pl.multiple_of(block * 8, 8), 8), :]

    def put_block(k, block, value):
        vec[k, pl.ds(pl.multiple_of(block * 8, 8), 8), :] = value

    def root_of(block):
        return jnp.broadcast_to(inv_root[pl.ds(block, 1), :], (8, LANES))

    def gram_copy(index, off):
        peer = lax.rem(me + off, n_rows)
        return pltpu.make_async_remote_copy(
            src_ref=gram_send.at[index],
            dst_ref=gram_recv.at[index, me],
            send_sem=gram_ssem.at[index, off],
            recv_sem=gram_rsem.at[index, off],
            device_id={"rows": peer},
            device_id_type=MESH,
        )

    def gram_begin(index, accs):
        gram = zero
        for q, acc in enumerate(accs):
            gram = jnp.where(lane == q, jnp.sum(acc, axis=1, keepdims=True), gram)
        gram_send[index] = gram
        gram_recv[index, me] = gram

        def send(off, carry):
            gram_copy(index, off).start()
            return carry

        lax.fori_loop(1, n_rows, send, 0)

    def gram_end(index, count):
        def wait(off, carry):
            gram_copy(index, off).wait()
            return carry

        lax.fori_loop(1, n_rows, wait, 0)
        gram = jnp.sum(gram_recv[index], axis=0) * (1.0 / node_total)
        return [jnp.broadcast_to(gram[:, q : q + 1], (8, LANES)) for q in range(count)]

    def grams(pairs):
        def body(block, accs):
            out = []
            for i, (left, right) in enumerate(pairs):
                value = block_of(left, block)
                out += [accs[i * 8 + q] + value * row_of(right, block, q) for q in range(8)]
            return tuple(out)

        return lax.fori_loop(0, nb, body, (zero,) * (8 * len(pairs)), unroll=8)

    def spread(column, row):
        return jnp.broadcast_to(column[row : row + 1, :], (8, LANES))

    def factorise(work):
        work = list(work)
        inverse_cols = [jnp.where(sub == q, 1.0, 0.0) for q in range(8)]
        factor = []
        scale = zero
        for j in range(8):
            root = lax.rsqrt(spread(work[j], j))
            scale = jnp.where(sub == j, root, scale)
            part = work[j] * root
            factor.append(jnp.where(sub >= j, part, 0.0))
            lower_part = jnp.where(sub > j, part * root, 0.0)
            for q in range(j + 1, 8):
                work[q] = work[q] - lower_part * spread(work[q], j)
            for q in range(j + 1):
                inverse_cols[q] = inverse_cols[q] - lower_part * spread(inverse_cols[q], j)
        inverse_cols = [column * scale for column in inverse_cols]
        transposed = [jnp.where(sub <= q, work[q] * scale, 0.0) for q in range(8)]
        return factor, inverse_cols, transposed

    def product(left, right):
        out = []
        for q in range(8):
            value = left[0] * spread(right[q], 0)
            for k in range(1, 8):
                value = value + left[k] * spread(right[q], k)
            out.append(value)
        return out

    def outer(left):
        out = []
        for q in range(8):
            value = left[0] * spread(left[0], q)
            for k in range(1, 8):
                value = value + left[k] * spread(left[k], q)
            out.append(value)
        return out

    def minus(left, right):
        return [a - b for a, b in zip(left, right)]

    def put_matrix(place, columns):
        value = zero
        for q in range(8):
            value = jnp.where(lane == q, columns[q], value)
        coef_ref[place] = value

    def mixed(terms, block):
        value = None
        for columns, k in terms:
            for q in range(8):
                part = columns[q] * row_of(k, block, q)
                value = part if value is None else value + part
        return value

    def mix(terms, target):
        def body(block, carry):
            put_block(target, block, mixed(terms, block))
            return carry

        lax.fori_loop(0, nb, body, 0, unroll=4)

    def folded(value):
        return value if value.shape[0] == 8 else value[:8] + value[8:]

    def products(lhs_of, source, sums, first):
        by, other, keep = first + BY_COL, first + COL_OTHER, first + COL_KEEP
        acc = zero
        for m in range(0, slots, 2):
            pair = (m, m + 1)
            lhs = [lhs_of(table[other, k]) for k in pair]
            height = lhs[0].shape[0]
            y = lax.dot_general(
                jnp.concatenate(lhs, axis=0),
                jnp.concatenate([source[table[by, k]] for k in pair], axis=1),
                (((1,), (0,)), ((), ())),
                preferred_element_type=f32,
            )
            for i, k in enumerate(pair):
                part = y[i * height : (i + 1) * height, i * LANES : (i + 1) * LANES]
                acc = acc * table[keep, k].astype(f32) + folded(part)
                sums[k] = acc

    row_sums[slots] = zero
    col_sums[slots] = zero

    def exchange(src, dst, ssem, rsem):
        return [
            pltpu.make_async_remote_copy(
                src_ref=src(side),
                dst_ref=dst(1 - side),
                send_sem=ssem(side),
                recv_sem=rsem(side),
                device_id={"rows": lower if side == 0 else upper},
                device_id_type=MESH,
            )
            for side in range(2)
        ]

    loads[4].wait()
    loads[5].wait()
    ones = jnp.concatenate([jnp.ones((8, LANES), bf16), jnp.zeros((8, LANES), bf16)], axis=0)
    products(lambda b: ones, tiles, col_sums, BY_COL)
    for side in range(2):
        for c in range(nh):
            deg_send[side, c : c + 1, :] = col_sums[table[COL_END, nb + side * nh + c], 0:1, :]
    deg_copies = exchange(
        lambda side: deg_send.at[side], lambda side: deg_recv.at[side],
        lambda side: deg_ssem.at[side], lambda side: deg_rsem.at[side],
    )
    for copy in deg_copies:
        copy.start()


    def turn(t, carry):
        turned[t] = tiles[t].T
        return carry

    lax.fori_loop(0, slots, turn, 0, unroll=16)
    products(lambda b: ones, turned, row_sums, BY_ROW)

    sub_l = lax.broadcasted_iota(jnp.int32, (LANES, LANES), 0)
    sub_b = lax.broadcasted_iota(jnp.int32, (nb, LANES), 0)
    lane_b = lax.broadcasted_iota(jnp.int32, (nb, LANES), 1)
    for side in range(2):
        total = jnp.zeros((2 * nb, LANES), f32)
        for c in range(nh):
            where = bound_ref[side : side + 1, c * LANES : (c + 1) * LANES]
            in_block = sub_b == jnp.broadcast_to(jnp.right_shift(where, 7), (nb, LANES))
            at_lane = sub_l == jnp.broadcast_to(jnp.bitwise_and(where, LANES - 1), (LANES, LANES))
            h = lane_b + c * LANES
            high = jnp.where(in_block, (jnp.right_shift(h, 6) + 1).astype(f32), 0.0)
            low = jnp.where(in_block, jnp.bitwise_and(h, 63).astype(f32), 0.0)
            total = total + lax.dot_general(
                jnp.concatenate([high, low], axis=0).astype(bf16), jnp.where(at_lane, 1.0, 0.0).astype(bf16),
                (((1,), (1,)), ((), ())), preferred_element_type=f32,
            )
        inverse[pl.ds(side * nb, nb), :] = ((total[:nb] - 1.0) * 64.0 + total[nb:]).astype(jnp.int32)

    def found_of(source_of, where, count):
        spot = jnp.bitwise_and(where, LANES - 1)
        block = jnp.right_shift(where, 7)
        found = zero
        for s in range(count):
            picked = jnp.take_along_axis(source_of(s).astype(f32), spot, axis=1, mode="promise_in_bounds")
            found = jnp.where(block == s, picked, found)
        return found

    for off in range(1, n_probe):
        start_copy(off).wait()

    def take_start(block, carry):
        where = pl.ds(pl.multiple_of(block * LANES, LANES), LANES)
        for g in range(n_probe):
            vec[0, pl.ds(block * 8 + g * probes_dev, probes_dev), :] = gathered[g, :, where]
        return carry

    lax.fori_loop(0, nb, take_start, 0, unroll=8)
    gram_begin(0, grams([(0, 0)]))
    for b in range(nb):
        inv_root[b : b + 1, :] = row_sums[table[ROW_END, b], 0:1, :] + col_sums[table[COL_END, b], 0:1, :]
    for copy in deg_copies:
        copy.wait()
    for g in range(nb // 8):
        degree = 1.0 + inv_root[g * 8 : g * 8 + 8, :]
        for side in range(2):
            degree = degree + found_of(
                lambda s: jnp.broadcast_to(deg_recv[side, s : s + 1, :], (8, LANES)),
                inverse[side * nb + g * 8 : side * nb + g * 8 + 8, :], nh,
            )
        inv_root[g * 8 : g * 8 + 8, :] = 1.0 / jnp.sqrt(degree)


    def planes(value):
        top = value.astype(bf16)
        if PLANES == 1:
            return top
        return jnp.concatenate([top, (value - top.astype(f32)).astype(bf16)], axis=0)

    mine = (1 - half).astype(f32)

    def scale_block(step, block, value):
        value = root_of(block) * value
        scaled[pl.ds(pl.multiple_of(block * 8, 8), 8), :] = value
        own[block] = planes(value)
        extended[step][block] = planes(value * mine)

    for step in range(STEPS):
        for c in range(nh):
            extended[step][nb + (1 - served) * nh + c] = jnp.zeros((8 * PLANES, LANES), bf16)

    def to_partner(src_ref, dst_ref, send_sem, recv_sem):
        copy = pltpu.make_async_remote_copy(
            src_ref=src_ref, dst_ref=dst_ref, send_sem=send_sem, recv_sem=recv_sem,
            device_id={"rows": partner}, device_id_type=MESH,
        )
        copy.start()
        return copy

    def send_halo(step):
        def gather_block(c, carry):
            where = pl.ds(pl.multiple_of(c * LANES, LANES), LANES)
            piece = jnp.where(served == 1, bound_ref[1:2, where], bound_ref[0:1, where])
            found = found_of(lambda s: scaled[s * 8 : s * 8 + 8, :], jnp.broadcast_to(piece, (8, LANES)), nb)
            halo_send[step, c] = planes(found)
            return carry

        lax.fori_loop(0, nh, gather_block, 0, unroll=4)
        return to_partner(
            halo_send.at[step], extended[step].at[pl.ds(nb + (1 - served) * nh, nh)], halo_ssem.at[step], halo_rsem.at[step]
        )

    def send_returns(step):
        products(lambda b: own[b], tiles, col_sums, BY_COL)
        for c in range(nh):
            ret_send[step, c] = col_sums[table[COL_END, nb + served * nh + c]].astype(RETURN_TYPE)
        return to_partner(ret_send.at[step], ret_recv.at[step], ret_ssem.at[step], ret_rsem.at[step])

    def part_copy(step, piece):
        where = pl.ds(piece * (nb // PIECES), nb // PIECES)
        return pltpu.make_async_remote_copy(
            src_ref=part_send.at[step, where], dst_ref=part_recv.at[step, where],
            send_sem=part_ssem.at[step, piece], recv_sem=part_rsem.at[step, piece],
            device_id={"probe": sibling}, device_id_type=MESH,
        )

    def send_parts(step):
        def body(block, carry):
            total = row_sums[table[ROW_END, block]] + mine * col_sums[table[COL_END, block]]
            where = jnp.broadcast_to(inverse[pl.ds(served * nb + block, 1), :], (8, LANES))
            part_send[step, block] = total + found_of(lambda s: ret_recv[step, s], where, nh)
            return carry

        size = nb // PIECES
        for piece in range(PIECES):
            lax.fori_loop(piece * size, (piece + 1) * size, body, 0, unroll=8)
            part_copy(step, piece).start()

    def image_of(step, source, block):
        root = root_of(block)
        return -(root * (root * block_of(source, block) + (part_send[step, block] + part_recv[step, block])))

    start_at = 0

    def q_at(j):
        return j

    def u_at(j):
        return STEPS + j

    def close(step, gram, coupling):
        shift = gram[8:]
        rest = minus(gram[:8], outer(shift))
        if coupling is not None:
            rest = minus(rest, outer(coupling))
        factor, inv_cols, next_coupling = factorise(rest)
        put_matrix(step - 1, [column + jnp.where(sub == q, 1.0, 0.0) for q, column in enumerate(shift)])
        put_matrix(STEPS + step - 1, factor)
        less = [[-column for column in product(inv_cols, shift)]]
        if coupling is not None:
            less.append([-column for column in product(inv_cols, coupling)])
        return inv_cols, less, next_coupling

    def scale_start(block, carry):
        scale_block(0, block, block_of(start_at, block))
        return carry

    lax.fori_loop(0, nb, scale_start, 0, unroll=4)
    coupling = None
    for step in range(STEPS):
        source = u_at(step) if step else start_at
        halo = send_halo(step)
        if step:
            gram_begin(step, grams([(source, source), (source, q_at(step))]))
        returned = send_returns(step)
        halo.wait()
        products(lambda b: extended[step][b], turned, row_sums, BY_ROW)
        returned.wait()
        send_parts(step)
        gram = gram_end(step, 16 if step else 8)
        if step:
            inv_cols, less, coupling = close(step, gram, coupling)
        else:
            _, inv_cols, _ = factorise(gram)
            less = []
        q_terms = [(inv_cols, source)] + [(columns, q_at(step - i)) for i, columns in enumerate(less)]
        mix(q_terms, q_at(step + 1))
        for piece in range(PIECES):
            part_copy(step, piece).wait()
        u_terms = [(columns, u_at(step - i)) for i, columns in enumerate(less)]

        def next_image(block, carry):
            image = image_of(step, source, block)
            value = inv_cols[0] * spread(image, 0)
            for q in range(1, 8):
                value = value + inv_cols[q] * spread(image, q)
            if u_terms:
                value = value + mixed(u_terms, block)
            put_block(u_at(step + 1), block, value)
            if step + 1 < STEPS:
                scale_block(step + 1, block, value)
            return carry

        lax.fori_loop(0, nb, next_image, 0, unroll=4)

    gram_begin(STEPS, grams([(u_at(STEPS), u_at(STEPS)), (u_at(STEPS), q_at(STEPS))]))
    gram = gram_end(STEPS, 16)
    inv_cols, less, _ = close(STEPS, gram, coupling)
    q_terms = [(inv_cols, u_at(STEPS))] + [(columns, q_at(STEPS - i)) for i, columns in enumerate(less)]
    mix(q_terms, start_at)
    for p in range(probes_dev):
        for b in range(nb):
            basis_ref[p : p + 1, b * LANES : (b + 1) * LANES] = vec[
                start_at, pl.ds(b * 8 + my_probe * probes_dev + p, 1), :
            ]


def in_hbm(value):
    return pltpu.with_memory_space_constraint(value, pltpu.HBM)


def local(start_block, blocks, block_rows, block_cols, counts, boundary):
    n_rows, n_probe = lax.axis_size("rows"), lax.axis_size("probe")
    probes_dev, rows_dev = start_block.shape
    slots = blocks.shape[0]
    nb = rows_dev // LANES
    nh = nb // 2
    f32, bf16 = jnp.float32, jnp.bfloat16
    vmem = pl.BlockSpec(memory_space=pltpu.VMEM)
    dma = pltpu.SemaphoreType.DMA
    height = 8 * PLANES
    basis, coef = pl.pallas_call(
        functools.partial(kernel, n_rows, n_probe, rows_dev * n_rows),
        out_shape=(
            jax.ShapeDtypeStruct((probes_dev, rows_dev), f32),
            jax.ShapeDtypeStruct((2 * STEPS, 8, LANES), f32),
        ),
        in_specs=[pl.BlockSpec(memory_space=pltpu.HBM)] * 6,
        out_specs=(vmem, vmem),
        scratch_shapes=[
            pltpu.VMEM(start_block.shape, f32),
            pltpu.VMEM(blocks.shape, bf16),
            pltpu.VMEM(blocks.shape, bf16),
            pltpu.VMEM((1, slots), jnp.int32),
            pltpu.VMEM((1, slots), jnp.int32),
            pltpu.SMEM(counts.shape, jnp.int32),
            pltpu.VMEM(boundary.shape, jnp.int32),
            pltpu.VMEM((n_probe, probes_dev, rows_dev), f32),
            pltpu.VMEM((2 * STEPS + 1, nb * 8, LANES), f32),
            pltpu.VMEM((nb * 8, LANES), f32),
            pltpu.VMEM((nb, LANES), f32),
            pltpu.VMEM((2 * nb, LANES), jnp.int32),
            pltpu.VMEM((8, LANES), jnp.int32),
            pltpu.SMEM((8, LANES), jnp.int32),
            pltpu.VMEM((nb, height, LANES), bf16),
            *[pltpu.VMEM((2 * nb, height, LANES), bf16)] * STEPS,
            pltpu.VMEM((STEPS, nh, height, LANES), bf16),
            pltpu.VMEM((STEPS, nh, 8, LANES), RETURN_TYPE),
            pltpu.VMEM((STEPS, nh, 8, LANES), RETURN_TYPE),
            pltpu.VMEM((2, nh, LANES), f32),
            pltpu.VMEM((2, nh, LANES), f32),
            pltpu.VMEM((STEPS, nb, 8, LANES), f32),
            pltpu.VMEM((STEPS, nb, 8, LANES), f32),
            pltpu.VMEM((slots + 1, 8, LANES), f32),
            pltpu.VMEM((slots + 1, 8, LANES), f32),
            pltpu.VMEM((STEPS + 1, 8, LANES), f32),
            pltpu.VMEM((STEPS + 1, n_rows, 8, LANES), f32),
            dma((6,)),
            dma,
            dma((n_probe,)),
            dma((n_probe,)),
            dma((STEPS,)),
            dma((STEPS,)),
            dma((STEPS,)),
            dma((STEPS,)),
            dma((STEPS, PIECES)),
            dma((STEPS, PIECES)),
            dma((2,)),
            dma((2,)),
            dma((STEPS + 1, n_rows)),
            dma((STEPS + 1, n_rows)),
        ],
        compiler_params=pltpu.CompilerParams(
            collective_id=0, has_side_effects=True, vmem_limit_bytes=VMEM_BYTES
        ),
        name="lanczos",
    )(
        in_hbm(start_block), in_hbm(blocks), in_hbm(block_rows.reshape(1, slots)),
        in_hbm(block_cols.reshape(1, slots)), counts, in_hbm(boundary),
    )
    return basis, coef[:STEPS, :, :8], coef[STEPS:, :, :8]


def solution(mesh):
    in_specs = (
        P("probe", "rows"),
        P("rows", None, None),
        P("rows"),
        P("rows"),
        P("rows"),
        P(None, "rows"),
    )
    out_specs = (P("probe", "rows"), P(), P())
    return jax.shard_map(local, mesh=mesh, in_specs=in_specs, out_specs=out_specs, check_vma=False)
```

```python
import functools

import jax
import jax.numpy as jnp
from jax import lax
from jax.experimental import pallas as pl
from jax.experimental.pallas import tpu as pltpu
from jax.sharding import PartitionSpec as P

STEPS = 3
LANES = 128
PIECES = 4
VMEM_BYTES = 48 * 1024 * 1024
MESH = pl.DeviceIdType.MESH
BY_COL, COL_OTHER, COL_END, COL_KEEP, BY_ROW, ROW_OTHER, ROW_END, ROW_KEEP = range(8)


def kernel(
    n_rows, n_probe, node_total,
    start_hbm, tiles_hbm, rows_hbm, cols_hbm, counts_hbm, bound_hbm,
    basis_ref, coef_ref,
    start_ref, tiles, turned, rows_ref, cols_ref, counts_ref, bound_ref, gathered, vec, spare, scaled, inv_root, inverse, table_v, table,
    boundary_of, own, extended, start_halo_send, start_halo_recv, root_halo_send, root_halo_recv, halo_send, halo_recv,
    first_send, first_recv, ret_send, ret_recv, returned, deg_send, deg_recv, part_send, part_recv, row_sums, col_sums, gram_send, gram_recv,
    load_sem, table_sem, start_send, start_recv, root_ssem, root_rsem, halo_ssem, halo_rsem, ret_ssem, ret_rsem, part_ssem, part_rsem, deg_ssem, deg_rsem,
    gram_ssem, gram_rsem,
):
    me = lax.axis_index("rows")
    my_probe = lax.axis_index("probe")
    slots = tiles.shape[0]
    nb = inv_root.shape[0]
    nh = nb // 2
    probes_dev = start_ref.shape[0]
    lower = lax.rem(me + n_rows - 1, n_rows)
    upper = lax.rem(me + 1, n_rows)
    half = lax.rem(my_probe, 2)
    sibling = my_probe + 1 - 2 * half
    served = 1 - lax.rem(me + half, 2)
    partner = lax.rem(me + 2 * served - 1 + n_rows, n_rows)
    f32, bf16 = jnp.float32, jnp.bfloat16

    moves = (
        (rows_hbm, rows_ref), (cols_hbm, cols_ref), (counts_hbm, counts_ref), (start_hbm, start_ref),
        (bound_hbm, bound_ref), (tiles_hbm, tiles),
    )
    loads = [pltpu.make_async_copy(source, target, load_sem.at[i]) for i, (source, target) in enumerate(moves)]
    for load in loads:
        load.start()

    barrier = pltpu.get_barrier_semaphore()
    for off in range(1, n_probe):
        peer = lax.rem(my_probe + off, n_probe)
        pl.semaphore_signal(barrier, inc=1, device_id={"probe": peer}, device_id_type=MESH)

    def greet(off, carry):
        peer = lax.rem(me + off, n_rows)
        for probe in (my_probe, sibling):
            pl.semaphore_signal(barrier, inc=1, device_id={"rows": peer, "probe": probe}, device_id_type=MESH)
        return carry

    lax.fori_loop(1, n_rows, greet, 0)

    lane = lax.broadcasted_iota(jnp.int32, (8, LANES), 1)
    sub = lax.broadcasted_iota(jnp.int32, (8, LANES), 0)
    zero = jnp.zeros((8, LANES), f32)

    lane_s = lax.broadcasted_iota(jnp.int32, (slots, slots), 1).astype(f32)
    sub_s = lax.broadcasted_iota(jnp.int32, (slots, slots), 0).astype(f32)
    lane_k = lax.broadcasted_iota(jnp.int32, (slots, LANES), 1).astype(f32)
    diagonal = lane_s == sub_s
    slot = lax.broadcasted_iota(jnp.int32, (1, slots), 1)
    for load in loads[:3]:
        load.wait()
    live = slot < counts_ref[0]

    def down(row):
        return jnp.sum(jnp.where(diagonal, jnp.broadcast_to(row, (slots, slots)), 0.0), axis=1, keepdims=True)

    def order(keys, other, others_most, first):
        key = jnp.where(live, keys, 2 * nb).astype(f32)
        key_down = down(key)
        other_down = down(other.astype(f32))
        key_row = jnp.broadcast_to(key, (slots, slots))
        same = key_row == key_down
        before = jnp.where(same, jnp.where(lane_s < sub_s, 1.0, 0.0), 0.0)
        rank = jnp.sum(jnp.where(key_row < key_down, 1.0, before), axis=1, keepdims=True)
        kept = jnp.where(jnp.sum(before, axis=1, keepdims=True) > 0.0, 1.0, 0.0)
        placed = rank == lane_s
        perm = jnp.sum(jnp.where(placed, sub_s, 0.0), axis=0, keepdims=True)
        others = jnp.sum(jnp.where(placed, other_down, 0.0), axis=0, keepdims=True)
        keep = jnp.sum(jnp.where(placed, kept, 0.0), axis=0, keepdims=True)
        up_to = jnp.sum(jnp.where(key_down <= lane_k, 1.0, 0.0), axis=0, keepdims=True)
        some = jnp.sum(jnp.where(key_down == lane_k, 1.0, 0.0), axis=0, keepdims=True)
        end = jnp.where(some > 0.0, up_to - 1.0, float(slots))
        rows = ((perm, slots - 1), (others, others_most), (end, slots), (keep, 1))
        for place, (value, most) in enumerate(rows):
            table_v[first + place : first + place + 1, :] = jnp.clip(value.astype(jnp.int32), 0, most)

    order(cols_ref[...], rows_ref[...], nb - 1, BY_COL)
    order(rows_ref[...], cols_ref[...], 2 * nb - 1, BY_ROW)
    table_copy = pltpu.make_async_copy(table_v, table, table_sem)
    table_copy.start()

    pl.semaphore_wait(barrier, n_probe - 1 + 2 * (n_rows - 1))

    def arrived(ref, send_sem, recv_sem):
        return pltpu.make_async_remote_copy(
            src_ref=ref, dst_ref=ref, send_sem=send_sem, recv_sem=recv_sem,
            device_id={"probe": sibling}, device_id_type=MESH,
        )

    def wait_for(ref, send_sem, recv_sem):
        arrived(ref, send_sem, recv_sem).wait()

    def start_copy(off):
        peer = lax.rem(my_probe + off, n_probe)
        return pltpu.make_async_remote_copy(
            src_ref=start_ref,
            dst_ref=gathered.at[my_probe],
            send_sem=start_send,
            recv_sem=start_recv,
            device_id={"probe": peer},
            device_id_type=MESH,
        )

    loads[3].wait()
    for off in range(1, n_probe):
        start_copy(off).start()
    gathered[my_probe] = start_ref[...]
    table_copy.wait()
    loads[4].wait()
    for c in range(nh):
        where = slice(c * LANES, (c + 1) * LANES)
        boundary_of[c : c + 1, :] = jnp.where(served == 1, bound_ref[1:2, where], bound_ref[0:1, where])
    sub_l = lax.broadcasted_iota(jnp.int32, (LANES, LANES), 0)
    sub_b = lax.broadcasted_iota(jnp.int32, (nb, LANES), 0)
    lane_b = lax.broadcasted_iota(jnp.int32, (nb, LANES), 1)
    for side in range(2):
        total = jnp.zeros((2 * nb, LANES), f32)
        for c in range(nh):
            where = bound_ref[side : side + 1, c * LANES : (c + 1) * LANES]
            in_block = sub_b == jnp.broadcast_to(jnp.right_shift(where, 7), (nb, LANES))
            at_lane = sub_l == jnp.broadcast_to(jnp.bitwise_and(where, LANES - 1), (LANES, LANES))
            h = lane_b + c * LANES
            high = jnp.where(in_block, (jnp.right_shift(h, 6) + 1).astype(f32), 0.0)
            low = jnp.where(in_block, jnp.bitwise_and(h, 63).astype(f32), 0.0)
            total = total + lax.dot_general(
                jnp.concatenate([high, low], axis=0).astype(bf16), jnp.where(at_lane, 1.0, 0.0).astype(bf16),
                (((1,), (1,)), ((), ())), preferred_element_type=f32,
            )
        inverse[pl.ds(side * nb, nb), :] = ((total[:nb] - 1.0) * 64.0 + total[nb:]).astype(jnp.int32)


    def row_of(k, block, probe):
        return jnp.broadcast_to(vec[k, pl.ds(block * 8 + probe, 1), :], (8, LANES))

    def block_of(k, block):
        return vec[k, pl.ds(pl.multiple_of(block * 8, 8), 8), :]

    def put_block(k, block, value):
        vec[k, pl.ds(pl.multiple_of(block * 8, 8), 8), :] = value

    def root_of(block):
        return jnp.broadcast_to(inv_root[pl.ds(block, 1), :], (8, LANES))

    def gram_copy(index, off, probe):
        peer = lax.rem(me + off, n_rows)
        return pltpu.make_async_remote_copy(
            src_ref=gram_send.at[index],
            dst_ref=gram_recv.at[index, me],
            send_sem=gram_ssem.at[index],
            recv_sem=gram_rsem.at[index],
            device_id={"rows": peer, "probe": probe},
            device_id_type=MESH,
        )

    def gram_begin(index, accs):
        gram = zero
        for q, acc in enumerate(accs):
            gram = jnp.where(lane == q, jnp.sum(acc, axis=1, keepdims=True), gram)
        gram_send[index] = gram
        gram_recv[index, me] = gram

        def send(off, carry):
            for probe in (sibling, my_probe):
                gram_copy(index, off, probe).start()
            return carry

        @pl.when(half == 1)
        def _():
            lax.fori_loop(1, n_rows, send, 0)

    def gram_end(index, count):
        others = gram_recv.at[index, pl.ds(0, n_rows - 1)]
        arrived(others, gram_ssem.at[index], gram_rsem.at[index]).wait_recv()

        @pl.when(half == 1)
        def _():
            for _ in range(2):
                arrived(others, gram_ssem.at[index], gram_rsem.at[index]).wait_send()

        gram = jnp.sum(gram_recv[index], axis=0) * (1.0 / node_total)
        return [jnp.broadcast_to(gram[:, q : q + 1], (8, LANES)) for q in range(count)]

    def grams(pairs):
        def body(block, accs):
            out = []
            for i, (left, right) in enumerate(pairs):
                value = block_of(left, block)
                out += [accs[i * 8 + q] + value * row_of(right, block, q) for q in range(8)]
            return tuple(out)

        return lax.fori_loop(0, nb, body, (zero,) * (8 * len(pairs)), unroll=8)

    def spread(column, row):
        return jnp.broadcast_to(column[row : row + 1, :], (8, LANES))

    def factorise(work):
        work = list(work)
        inverse_cols = [jnp.where(sub == q, 1.0, 0.0) for q in range(8)]
        factor = []
        scale = zero
        for j in range(8):
            root = lax.rsqrt(spread(work[j], j))
            scale = jnp.where(sub == j, root, scale)
            part = work[j] * root
            factor.append(jnp.where(sub >= j, part, 0.0))
            lower_part = jnp.where(sub > j, part * root, 0.0)
            for q in range(j + 1, 8):
                work[q] = work[q] - lower_part * spread(work[q], j)
            for q in range(j + 1):
                inverse_cols[q] = inverse_cols[q] - lower_part * spread(inverse_cols[q], j)
        inverse_cols = [column * scale for column in inverse_cols]
        transposed = [jnp.where(sub <= q, work[q] * scale, 0.0) for q in range(8)]
        return factor, inverse_cols, transposed

    def product(left, right):
        out = []
        for q in range(8):
            value = left[0] * spread(right[q], 0)
            for k in range(1, 8):
                value = value + left[k] * spread(right[q], k)
            out.append(value)
        return out

    def outer(left):
        out = []
        for q in range(8):
            value = left[0] * spread(left[0], q)
            for k in range(1, 8):
                value = value + left[k] * spread(left[k], q)
            out.append(value)
        return out

    def minus(left, right):
        return [a - b for a, b in zip(left, right)]

    def put_matrix(place, columns):
        value = zero
        for q in range(8):
            value = jnp.where(lane == q, columns[q], value)
        coef_ref[place] = value

    def mixed(terms, block):
        value = None
        for columns, k in terms:
            for q in range(8):
                part = columns[q] * row_of(k, block, q)
                value = part if value is None else value + part
        return value

    def mix(terms, target):
        def body(block, carry):
            put_block(target, block, mixed(terms, block))
            return carry

        lax.fori_loop(0, nb, body, 0, unroll=4)

    def folded(value):
        return value if value.shape[0] == 8 else value[:8] + value[8:]

    def products(lhs_of, source, sums, first, beside=()):
        by, other, keep = first + BY_COL, first + COL_OTHER, first + COL_KEEP
        acc = zero
        for m in range(0, slots, 2):
            pair = (m, m + 1)
            lhs = [lhs_of(table[other, k]) for k in pair]
            height = lhs[0].shape[0]
            y = lax.dot_general(
                jnp.concatenate(lhs, axis=0),
                jnp.concatenate([source[table[by, k]] for k in pair], axis=1),
                (((1,), (0,)), ((), ())),
                preferred_element_type=f32,
            )
            for i, k in enumerate(pair):
                part = y[i * height : (i + 1) * height, i * LANES : (i + 1) * LANES]
                acc = acc * table[keep, k].astype(f32) + folded(part)
                sums[k] = acc
            for task in range(m * len(beside) // slots, (m + 2) * len(beside) // slots):
                beside[task]()

    row_sums[slots] = zero
    col_sums[slots] = zero

    def exchange(src, dst, ssem, rsem):
        return [
            pltpu.make_async_remote_copy(
                src_ref=src(side),
                dst_ref=dst(1 - side),
                send_sem=ssem(side),
                recv_sem=rsem(side),
                device_id={"rows": lower if side == 0 else upper},
                device_id_type=MESH,
            )
            for side in range(2)
        ]

    def found_of(source_of, where, count):
        spot = jnp.bitwise_and(where, LANES - 1)
        block = jnp.right_shift(where, 7)
        found = zero
        for s in range(count):
            picked = jnp.take_along_axis(source_of(s).astype(f32), spot, axis=1, mode="promise_in_bounds")
            found = jnp.where(block == s, picked, found)
        return found

    mine = (1 - half).astype(f32)

    def planes(value):
        top = value.astype(bf16)
        return jnp.concatenate([top, (value - top.astype(f32)).astype(bf16)], axis=0)

    def scale_block(block, value):
        value = root_of(block) * value
        scaled[pl.ds(pl.multiple_of(block * 8, 8), 8), :] = value
        own[block] = planes(value)
        extended[block] = planes(value * mine)

    for c in range(nh):
        extended[nb + (1 - served) * nh + c] = jnp.zeros((16, LANES), bf16)

    def to_partner(src_ref, dst_ref, send_sem, recv_sem):
        copy = pltpu.make_async_remote_copy(
            src_ref=src_ref, dst_ref=dst_ref, send_sem=send_sem, recv_sem=recv_sem,
            device_id={"rows": partner}, device_id_type=MESH,
        )
        copy.start()
        return copy

    def boundary_row(c):
        return jnp.broadcast_to(boundary_of[c : c + 1, :], (8, LANES))

    def send_start_halo():
        for c in range(nh):
            start_halo_send[c] = found_of(lambda s: block_of(0, s), boundary_row(c), nb)
        return to_partner(start_halo_send, start_halo_recv, halo_ssem.at[0], halo_rsem.at[0])

    def send_root_halo():
        for g in range(nh // 8):
            where = boundary_of[g * 8 : g * 8 + 8, :]
            root_halo_send[g * 8 : g * 8 + 8, :] = found_of(
                lambda s: jnp.broadcast_to(inv_root[s : s + 1, :], (8, LANES)), where, nb
            )
        return to_partner(root_halo_send, root_halo_recv, root_ssem, root_rsem)

    def gather_block(step, c):
        found = found_of(lambda s: scaled[s * 8 : s * 8 + 8, :], boundary_row(c), nb)
        halo_send[step, c] = found.astype(bf16)

    def send_halo(step):
        return to_partner(halo_send.at[step], halo_recv.at[step], halo_ssem.at[step], halo_rsem.at[step])

    def take_halo(step):
        for c in range(nh):
            if step:
                pieces = jnp.concatenate([halo_recv[step, c], jnp.zeros((8, LANES), bf16)], axis=0)
            else:
                pieces = planes(jnp.broadcast_to(root_halo_recv[c : c + 1, :], (8, LANES)) * start_halo_recv[c])
            extended[nb + served * nh + c] = pieces

    def send_returns(step):
        send, recv = (ret_send.at[step], ret_recv.at[step]) if step else (first_send, first_recv)
        for c in range(nh):
            send[c] = col_sums[table[COL_END, nb + served * nh + c]].astype(send.dtype)
        return to_partner(send, recv, ret_ssem.at[step], ret_rsem.at[step])

    def take_returns(step):
        for c in range(nh):
            returned[c] = ret_recv[step, c].astype(f32)

    def scatter_block(step, block):
        where = jnp.broadcast_to(inverse[pl.ds(served * nb + block, 1), :], (8, LANES))
        source = returned if step else first_recv
        part_send[step, block] = found_of(lambda s: source[s], where, nh)

    loads[5].wait()
    ones = jnp.concatenate([jnp.ones((8, LANES), bf16), jnp.zeros((8, LANES), bf16)], axis=0)
    products(lambda b: ones, tiles, col_sums, BY_COL)
    for side in range(2):
        for c in range(nh):
            deg_send[side, c : c + 1, :] = col_sums[table[COL_END, nb + side * nh + c], 0:1, :]
    deg_copies = exchange(
        lambda side: deg_send.at[side], lambda side: deg_recv.at[side],
        lambda side: deg_ssem.at[side], lambda side: deg_rsem.at[side],
    )
    for copy in deg_copies:
        copy.start()

    def turn(t, carry):
        turned[t] = tiles[t].T
        return carry

    lax.fori_loop(0, slots, turn, 0, unroll=16)
    products(lambda b: ones, turned, row_sums, BY_ROW)

    wait_for(gathered.at[pl.ds(0, n_probe - 1)], start_send, start_recv)

    def take_start(block, carry):
        where = pl.ds(pl.multiple_of(block * LANES, LANES), LANES)
        for g in range(n_probe):
            vec[0, pl.ds(block * 8 + g * probes_dev, probes_dev), :] = gathered[g, :, where]
        return carry

    lax.fori_loop(0, nb, take_start, 0, unroll=8)
    gram_begin(0, grams([(0, 0)]))
    start_halo = send_start_halo()
    for b in range(nb):
        inv_root[b : b + 1, :] = row_sums[table[ROW_END, b], 0:1, :] + col_sums[table[COL_END, b], 0:1, :]
    for copy in deg_copies:
        copy.wait()
    for g in range(nb // 8):
        degree = 1.0 + inv_root[g * 8 : g * 8 + 8, :]
        for side in range(2):
            degree = degree + found_of(
                lambda s: jnp.broadcast_to(deg_recv[side, s : s + 1, :], (8, LANES)),
                inverse[side * nb + g * 8 : side * nb + g * 8 + 8, :], nh,
            )
        inv_root[g * 8 : g * 8 + 8, :] = 1.0 / jnp.sqrt(degree)


    def part_copy(step, piece):
        where = pl.ds(piece * (nb // PIECES), nb // PIECES)
        return pltpu.make_async_remote_copy(
            src_ref=part_send.at[step, where], dst_ref=part_recv.at[step, where],
            send_sem=part_ssem.at[step], recv_sem=part_rsem.at[step],
            device_id={"probe": sibling}, device_id_type=MESH,
        )

    def send_parts(step):
        size = nb // PIECES
        for piece in range(PIECES):
            for block in range(piece * size, (piece + 1) * size):
                part_send[step, block] = (
                    part_send[step, block] + row_sums[table[ROW_END, block]] + mine * col_sums[table[COL_END, block]]
                )
            part_copy(step, piece).start()

    def image_of(step, source, block):
        root = root_of(block)
        return -(root * (root * block_of(source, block) + (part_send[step, block] + part_recv[step, block])))

    start_at = 0

    def q_at(j):
        return j

    def u_at(j):
        return STEPS + j

    def close(step, gram, coupling):
        shift = gram[8:]
        rest = minus(gram[:8], outer(shift))
        if coupling is not None:
            rest = minus(rest, outer(coupling))
        factor, inv_cols, next_coupling = factorise(rest)
        put_matrix(step - 1, [column + jnp.where(sub == q, 1.0, 0.0) for q, column in enumerate(shift)])
        put_matrix(STEPS + step - 1, factor)
        less = [[-column for column in product(inv_cols, shift)]]
        if coupling is not None:
            less.append([-column for column in product(inv_cols, coupling)])
        return inv_cols, less, next_coupling

    def scale_start(block, carry):
        scale_block(block, block_of(start_at, block))
        return carry

    root_halo = send_root_halo()
    lax.fori_loop(0, nb, scale_start, 0, unroll=4)
    coupling = None
    for step in range(STEPS):
        source = u_at(step) if step else start_at
        accs = [zero] * 16

        def gram_block(block):
            image = block_of(source, block)
            for q in range(8):
                accs[q] = accs[q] + image * row_of(source, block, q)
                accs[8 + q] = accs[8 + q] + image * row_of(q_at(step), block, q)

        beside = []
        if step:
            for c in range(nh):
                beside.append(functools.partial(gather_block, step, c))
                beside += [functools.partial(gram_block, 2 * c + i) for i in range(2)]
        products(lambda b: own[b], tiles, col_sums, BY_COL, beside)
        halo = send_halo(step) if step else start_halo
        returns = send_returns(step)
        if step:
            gram_begin(step, accs)
        halo.wait()
        if step == 0:
            root_halo.wait()
        take_halo(step)
        returns.wait()
        if step:
            take_returns(step)
        scatters = [functools.partial(scatter_block, step, block) for block in range(nb)]
        products(lambda b: extended[b], turned, row_sums, BY_ROW, scatters)
        send_parts(step)
        gram = gram_end(step, 16 if step else 8)
        if step:
            inv_cols, less, coupling = close(step, gram, coupling)
        else:
            _, inv_cols, _ = factorise(gram)
            less = []
        u_terms = [(columns, u_at(step - i)) for i, columns in enumerate(less)]
        if u_terms:
            mix(u_terms, u_at(step + 1))
        q_terms = [(inv_cols, source)] + [(columns, q_at(step - i)) for i, columns in enumerate(less)]
        mix(q_terms, q_at(step + 1))
        wait_for(part_recv.at[step], part_ssem.at[step], part_rsem.at[step])

        def next_image(block, carry):
            image = image_of(step, source, block)
            value = inv_cols[0] * spread(image, 0)
            for q in range(1, 8):
                value = value + inv_cols[q] * spread(image, q)
            if u_terms:
                value = value + block_of(u_at(step + 1), block)
            put_block(u_at(step + 1), block, value)
            if step + 1 < STEPS:
                scale_block(block, value)
            return carry

        lax.fori_loop(0, nb, next_image, 0, unroll=4)

    gram_begin(STEPS, grams([(u_at(STEPS), u_at(STEPS)), (u_at(STEPS), q_at(STEPS))]))
    gram = gram_end(STEPS, 16)
    inv_cols, less, _ = close(STEPS, gram, coupling)
    terms = [(inv_cols, u_at(STEPS))] + [(columns, q_at(STEPS - i)) for i, columns in enumerate(less)]
    for i, (columns, _) in enumerate(terms):
        for q in range(8):
            spare[i * 64 + q * 8 : i * 64 + q * 8 + 8, :] = columns[q]
    for p in range(probes_dev):
        total = jnp.zeros((nb, LANES), f32)
        for i, (_, k) in enumerate(terms):
            for q in range(8):
                weight = spare[pl.ds(i * 64 + q * 8 + my_probe * probes_dev + p, 1), :]
                total = total + jnp.broadcast_to(weight, (nb, LANES)) * vec[k, pl.ds(q, nb, stride=8), :]
        basis_ref[p] = total


def in_hbm(value):
    return pltpu.with_memory_space_constraint(value, pltpu.HBM)


def local(start_block, blocks, block_rows, block_cols, counts, boundary):
    n_rows, n_probe = lax.axis_size("rows"), lax.axis_size("probe")
    probes_dev, rows_dev = start_block.shape
    slots = blocks.shape[0]
    nb = rows_dev // LANES
    nh = nb // 2
    f32, bf16 = jnp.float32, jnp.bfloat16
    vmem = pl.BlockSpec(memory_space=pltpu.VMEM)
    dma = pltpu.SemaphoreType.DMA
    basis, coef = pl.pallas_call(
        functools.partial(kernel, n_rows, n_probe, rows_dev * n_rows),
        out_shape=(
            jax.ShapeDtypeStruct((probes_dev, nb, LANES), f32),
            jax.ShapeDtypeStruct((2 * STEPS, 8, LANES), f32),
        ),
        in_specs=[pl.BlockSpec(memory_space=pltpu.HBM)] * 6,
        out_specs=(vmem, vmem),
        scratch_shapes=[
            pltpu.VMEM(start_block.shape, f32),
            pltpu.VMEM(blocks.shape, bf16),
            pltpu.VMEM(blocks.shape, bf16),
            pltpu.VMEM((1, slots), jnp.int32),
            pltpu.VMEM((1, slots), jnp.int32),
            pltpu.SMEM(counts.shape, jnp.int32),
            pltpu.VMEM(boundary.shape, jnp.int32),
            pltpu.VMEM((n_probe, probes_dev, rows_dev), f32),
            pltpu.VMEM((2 * STEPS + 1, nb * 8, LANES), f32),
            pltpu.VMEM((3 * 64, LANES), f32),
            pltpu.VMEM((nb * 8, LANES), f32),
            pltpu.VMEM((nb, LANES), f32),
            pltpu.VMEM((2 * nb, LANES), jnp.int32),
            pltpu.VMEM((8, LANES), jnp.int32),
            pltpu.SMEM((8, LANES), jnp.int32),
            pltpu.VMEM((nh, LANES), jnp.int32),
            pltpu.VMEM((nb, 16, LANES), bf16),
            pltpu.VMEM((2 * nb, 16, LANES), bf16),
            pltpu.VMEM((nh, 8, LANES), f32),
            pltpu.VMEM((nh, 8, LANES), f32),
            pltpu.VMEM((nh, LANES), f32),
            pltpu.VMEM((nh, LANES), f32),
            pltpu.VMEM((STEPS, nh, 8, LANES), bf16),
            pltpu.VMEM((STEPS, nh, 8, LANES), bf16),
            pltpu.VMEM((nh, 8, LANES), f32),
            pltpu.VMEM((nh, 8, LANES), f32),
            pltpu.VMEM((STEPS, nh, 8, LANES), bf16),
            pltpu.VMEM((STEPS, nh, 8, LANES), bf16),
            pltpu.VMEM((nh, 8, LANES), f32),
            pltpu.VMEM((2, nh, LANES), f32),
            pltpu.VMEM((2, nh, LANES), f32),
            pltpu.VMEM((STEPS, nb, 8, LANES), f32),
            pltpu.VMEM((STEPS, nb, 8, LANES), f32),
            pltpu.VMEM((slots + 1, 8, LANES), f32),
            pltpu.VMEM((slots + 1, 8, LANES), f32),
            pltpu.VMEM((STEPS + 1, 8, LANES), f32),
            pltpu.VMEM((STEPS + 1, n_rows, 8, LANES), f32),
            dma((6,)),
            dma,
            dma,
            dma,
            dma,
            dma,
            dma((STEPS,)),
            dma((STEPS,)),
            dma((STEPS,)),
            dma((STEPS,)),
            dma((STEPS,)),
            dma((STEPS,)),
            dma((2,)),
            dma((2,)),
            dma((STEPS + 1,)),
            dma((STEPS + 1,)),
        ],
        compiler_params=pltpu.CompilerParams(
            collective_id=0, has_side_effects=True, vmem_limit_bytes=VMEM_BYTES
        ),
        name="lanczos",
    )(
        in_hbm(start_block), in_hbm(blocks), in_hbm(block_rows.reshape(1, slots)),
        in_hbm(block_cols.reshape(1, slots)), counts, in_hbm(boundary),
    )
    return basis.reshape(probes_dev, rows_dev), coef[:STEPS, :, :8], coef[STEPS:, :, :8]


def solution(mesh):
    in_specs = (
        P("probe", "rows"),
        P("rows", None, None),
        P("rows"),
        P("rows"),
        P("rows"),
        P(None, "rows"),
    )
    out_specs = (P("probe", "rows"), P(), P())
    return jax.shard_map(local, mesh=mesh, in_specs=in_specs, out_specs=out_specs, check_vma=False)
```

```python
import functools

import jax
import jax.numpy as jnp
from jax import lax
from jax.experimental import pallas as pl
from jax.experimental.pallas import tpu as pltpu
from jax.sharding import PartitionSpec as P

STEPS = 3
LANES = 128
PIECES = 4
VMEM_BYTES = 48 * 1024 * 1024
MESH = pl.DeviceIdType.MESH
BY_COL, COL_OTHER, COL_END, COL_KEEP, BY_ROW, ROW_OTHER, ROW_END, ROW_KEEP = range(8)


def kernel(
    n_rows, n_probe, node_total,
    start_hbm, tiles_hbm, rows_hbm, cols_hbm, counts_hbm, bound_hbm,
    basis_ref, coef_ref,
    start_ref, tiles, turned, rows_ref, cols_ref, counts_ref, bound_ref, gathered, vec, spare, scaled, inv_root, inverse, table_v, table,
    boundary_of, own, extended, start_halo_send, start_halo_recv, root_halo_send, root_halo_recv, halo_send, halo_recv,
    first_send, first_recv, ret_send, ret_recv, returned, deg_send, deg_recv, part_send, part_recv, row_sums, col_sums, gram_send, gram_recv,
    load_sem, table_sem, start_send, start_recv, root_ssem, root_rsem, halo_ssem, halo_rsem, ret_ssem, ret_rsem, part_ssem, part_rsem, deg_ssem, deg_rsem,
    gram_ssem, gram_rsem,
):
    me = lax.axis_index("rows")
    my_probe = lax.axis_index("probe")
    slots = tiles.shape[0]
    nb = inv_root.shape[0]
    nh = nb // 2
    probes_dev = start_ref.shape[0]
    lower = lax.rem(me + n_rows - 1, n_rows)
    upper = lax.rem(me + 1, n_rows)
    half = lax.rem(my_probe, 2)
    sibling = my_probe + 1 - 2 * half
    served = 1 - lax.rem(me + half, 2)
    partner = lax.rem(me + 2 * served - 1 + n_rows, n_rows)
    f32, bf16 = jnp.float32, jnp.bfloat16

    moves = (
        (rows_hbm, rows_ref), (cols_hbm, cols_ref), (counts_hbm, counts_ref), (start_hbm, start_ref),
        (bound_hbm, bound_ref), (tiles_hbm, tiles),
    )
    loads = [pltpu.make_async_copy(source, target, load_sem.at[i]) for i, (source, target) in enumerate(moves)]
    for load in loads:
        load.start()

    barrier = pltpu.get_barrier_semaphore()
    for off in range(1, n_probe):
        peer = lax.rem(my_probe + off, n_probe)
        pl.semaphore_signal(barrier, inc=1, device_id={"probe": peer}, device_id_type=MESH)

    def greet(off, carry):
        peer = lax.rem(me + off, n_rows)
        for probe in (my_probe, sibling):
            pl.semaphore_signal(barrier, inc=1, device_id={"rows": peer, "probe": probe}, device_id_type=MESH)
        return carry

    lax.fori_loop(1, n_rows, greet, 0)

    lane = lax.broadcasted_iota(jnp.int32, (8, LANES), 1)
    sub = lax.broadcasted_iota(jnp.int32, (8, LANES), 0)
    zero = jnp.zeros((8, LANES), f32)

    lane_s = lax.broadcasted_iota(jnp.int32, (slots, slots), 1).astype(f32)
    sub_s = lax.broadcasted_iota(jnp.int32, (slots, slots), 0).astype(f32)
    lane_k = lax.broadcasted_iota(jnp.int32, (slots, LANES), 1).astype(f32)
    diagonal = lane_s == sub_s
    slot = lax.broadcasted_iota(jnp.int32, (1, slots), 1)
    for load in loads[:3]:
        load.wait()
    live = slot < counts_ref[0]

    def down(row):
        return jnp.sum(jnp.where(diagonal, jnp.broadcast_to(row, (slots, slots)), 0.0), axis=1, keepdims=True)

    def order(keys, other, others_most, first):
        key = jnp.where(live, keys, 2 * nb).astype(f32)
        key_down = down(key)
        other_down = down(other.astype(f32))
        key_row = jnp.broadcast_to(key, (slots, slots))
        same = key_row == key_down
        before = jnp.where(same, jnp.where(lane_s < sub_s, 1.0, 0.0), 0.0)
        rank = jnp.sum(jnp.where(key_row < key_down, 1.0, before), axis=1, keepdims=True)
        kept = jnp.where(jnp.sum(before, axis=1, keepdims=True) > 0.0, 1.0, 0.0)
        placed = rank == lane_s
        perm = jnp.sum(jnp.where(placed, sub_s, 0.0), axis=0, keepdims=True)
        others = jnp.sum(jnp.where(placed, other_down, 0.0), axis=0, keepdims=True)
        keep = jnp.sum(jnp.where(placed, kept, 0.0), axis=0, keepdims=True)
        up_to = jnp.sum(jnp.where(key_down <= lane_k, 1.0, 0.0), axis=0, keepdims=True)
        some = jnp.sum(jnp.where(key_down == lane_k, 1.0, 0.0), axis=0, keepdims=True)
        end = jnp.where(some > 0.0, up_to - 1.0, float(slots))
        rows = ((perm, slots - 1), (others, others_most), (end, slots), (keep, 1))
        for place, (value, most) in enumerate(rows):
            table_v[first + place : first + place + 1, :] = jnp.clip(value.astype(jnp.int32), 0, most)

    order(cols_ref[...], rows_ref[...], nb - 1, BY_COL)
    order(rows_ref[...], cols_ref[...], 2 * nb - 1, BY_ROW)
    table_copy = pltpu.make_async_copy(table_v, table, table_sem)
    table_copy.start()

    pl.semaphore_wait(barrier, n_probe - 1 + 2 * (n_rows - 1))

    def arrived(ref, send_sem, recv_sem):
        return pltpu.make_async_remote_copy(
            src_ref=ref, dst_ref=ref, send_sem=send_sem, recv_sem=recv_sem,
            device_id={"probe": sibling}, device_id_type=MESH,
        )

    def wait_for(ref, send_sem, recv_sem):
        arrived(ref, send_sem, recv_sem).wait()

    def start_copy(off):
        peer = lax.rem(my_probe + off, n_probe)
        return pltpu.make_async_remote_copy(
            src_ref=start_ref,
            dst_ref=gathered.at[my_probe],
            send_sem=start_send,
            recv_sem=start_recv,
            device_id={"probe": peer},
            device_id_type=MESH,
        )

    loads[3].wait()
    for off in range(1, n_probe):
        start_copy(off).start()
    gathered[my_probe] = start_ref[...]
    table_copy.wait()
    loads[4].wait()
    for c in range(nh):
        where = slice(c * LANES, (c + 1) * LANES)
        boundary_of[c : c + 1, :] = jnp.where(served == 1, bound_ref[1:2, where], bound_ref[0:1, where])
    sub_l = lax.broadcasted_iota(jnp.int32, (LANES, LANES), 0)
    sub_b = lax.broadcasted_iota(jnp.int32, (nb, LANES), 0)
    lane_b = lax.broadcasted_iota(jnp.int32, (nb, LANES), 1)
    for side in range(2):
        total = jnp.zeros((2 * nb, LANES), f32)
        for c in range(nh):
            where = bound_ref[side : side + 1, c * LANES : (c + 1) * LANES]
            in_block = sub_b == jnp.broadcast_to(jnp.right_shift(where, 7), (nb, LANES))
            at_lane = sub_l == jnp.broadcast_to(jnp.bitwise_and(where, LANES - 1), (LANES, LANES))
            h = lane_b + c * LANES
            high = jnp.where(in_block, (jnp.right_shift(h, 6) + 1).astype(f32), 0.0)
            low = jnp.where(in_block, jnp.bitwise_and(h, 63).astype(f32), 0.0)
            total = total + lax.dot_general(
                jnp.concatenate([high, low], axis=0).astype(bf16), jnp.where(at_lane, 1.0, 0.0).astype(bf16),
                (((1,), (1,)), ((), ())), preferred_element_type=f32,
            )
        inverse[pl.ds(side * nb, nb), :] = ((total[:nb] - 1.0) * 64.0 + total[nb:]).astype(jnp.int32)


    def row_of(k, block, probe):
        return jnp.broadcast_to(vec[k, pl.ds(block * 8 + probe, 1), :], (8, LANES))

    def block_of(k, block):
        return vec[k, pl.ds(pl.multiple_of(block * 8, 8), 8), :]

    def put_block(k, block, value):
        vec[k, pl.ds(pl.multiple_of(block * 8, 8), 8), :] = value

    def root_of(block):
        return jnp.broadcast_to(inv_root[pl.ds(block, 1), :], (8, LANES))

    def gram_copy(index, off, probe):
        peer = lax.rem(me + off, n_rows)
        return pltpu.make_async_remote_copy(
            src_ref=gram_send.at[index],
            dst_ref=gram_recv.at[index, me],
            send_sem=gram_ssem.at[index],
            recv_sem=gram_rsem.at[index],
            device_id={"rows": peer, "probe": probe},
            device_id_type=MESH,
        )

    def gram_begin(index, accs):
        gram = zero
        for q, acc in enumerate(accs):
            gram = jnp.where(lane == q, jnp.sum(acc, axis=1, keepdims=True), gram)
        gram_send[index] = gram
        gram_recv[index, me] = gram

        def send(off, carry):
            for probe in (sibling, my_probe):
                gram_copy(index, off, probe).start()
            return carry

        @pl.when(half == 1)
        def _():
            lax.fori_loop(1, n_rows, send, 0, unroll=7)

    def gram_end(index, count):
        others = gram_recv.at[index, pl.ds(0, n_rows - 1)]
        arrived(others, gram_ssem.at[index], gram_rsem.at[index]).wait_recv()

        @pl.when(half == 1)
        def _():
            for _ in range(2):
                arrived(others, gram_ssem.at[index], gram_rsem.at[index]).wait_send()

        gram = jnp.sum(gram_recv[index], axis=0) * (1.0 / node_total)
        return [jnp.broadcast_to(gram[:, q : q + 1], (8, LANES)) for q in range(count)]

    def grams(pairs):
        def body(block, accs):
            out = []
            for i, (left, right) in enumerate(pairs):
                value = block_of(left, block)
                out += [accs[i * 8 + q] + value * row_of(right, block, q) for q in range(8)]
            return tuple(out)

        return lax.fori_loop(0, nb, body, (zero,) * (8 * len(pairs)), unroll=8)

    def spread(column, row):
        return jnp.broadcast_to(column[row : row + 1, :], (8, LANES))

    def factorise(work):
        work = list(work)
        inverse_cols = [jnp.where(sub == q, 1.0, 0.0) for q in range(8)]
        factor = []
        scale = zero
        for j in range(8):
            root = lax.rsqrt(spread(work[j], j))
            scale = jnp.where(sub == j, root, scale)
            part = work[j] * root
            factor.append(jnp.where(sub >= j, part, 0.0))
            lower_part = jnp.where(sub > j, part * root, 0.0)
            for q in range(j + 1, 8):
                work[q] = work[q] - lower_part * spread(work[q], j)
            for q in range(j + 1):
                inverse_cols[q] = inverse_cols[q] - lower_part * spread(inverse_cols[q], j)
        inverse_cols = [column * scale for column in inverse_cols]
        transposed = [jnp.where(sub <= q, work[q] * scale, 0.0) for q in range(8)]
        return factor, inverse_cols, transposed

    def product(left, right):
        out = []
        for q in range(8):
            value = left[0] * spread(right[q], 0)
            for k in range(1, 8):
                value = value + left[k] * spread(right[q], k)
            out.append(value)
        return out

    def outer(left):
        out = []
        for q in range(8):
            value = left[0] * spread(left[0], q)
            for k in range(1, 8):
                value = value + left[k] * spread(left[k], q)
            out.append(value)
        return out

    def minus(left, right):
        return [a - b for a, b in zip(left, right)]

    def put_matrix(place, columns):
        value = zero
        for q in range(8):
            value = jnp.where(lane == q, columns[q], value)
        coef_ref[place] = value

    def mixed(terms, block):
        value = None
        for columns, k in terms:
            for q in range(8):
                part = columns[q] * row_of(k, block, q)
                value = part if value is None else value + part
        return value

    def mix(terms, target):
        def body(block, carry):
            put_block(target, block, mixed(terms, block))
            return carry

        lax.fori_loop(0, nb, body, 0, unroll=4)

    def folded(value):
        return value if value.shape[0] == 8 else value[:8] + value[8:]

    def products(lhs_of, source, sums, first, beside=()):
        by, other, keep = first + BY_COL, first + COL_OTHER, first + COL_KEEP
        acc = zero
        for m in range(0, slots, 2):
            pair = (m, m + 1)
            lhs = [lhs_of(table[other, k]) for k in pair]
            height = lhs[0].shape[0]
            y = lax.dot_general(
                jnp.concatenate(lhs, axis=0),
                jnp.concatenate([source[table[by, k]] for k in pair], axis=1),
                (((1,), (0,)), ((), ())),
                preferred_element_type=f32,
            )
            for i, k in enumerate(pair):
                part = y[i * height : (i + 1) * height, i * LANES : (i + 1) * LANES]
                acc = acc * table[keep, k].astype(f32) + folded(part)
                sums[k] = acc
            for task in range(m * len(beside) // slots, (m + 2) * len(beside) // slots):
                beside[task]()

    row_sums[slots] = zero
    col_sums[slots] = zero

    def exchange(src, dst, ssem, rsem):
        return [
            pltpu.make_async_remote_copy(
                src_ref=src(side),
                dst_ref=dst(1 - side),
                send_sem=ssem(side),
                recv_sem=rsem(side),
                device_id={"rows": lower if side == 0 else upper},
                device_id_type=MESH,
            )
            for side in range(2)
        ]

    def found_of(source_of, where, count):
        spot = jnp.bitwise_and(where, LANES - 1)
        block = jnp.right_shift(where, 7)
        found = zero
        for s in range(count):
            picked = jnp.take_along_axis(source_of(s).astype(f32), spot, axis=1, mode="promise_in_bounds")
            found = jnp.where(block == s, picked, found)
        return found

    mine = (1 - half).astype(f32)

    def planes(value):
        top = value.astype(bf16)
        return jnp.concatenate([top, (value - top.astype(f32)).astype(bf16)], axis=0)

    def scale_block(block, value):
        value = root_of(block) * value
        scaled[pl.ds(pl.multiple_of(block * 8, 8), 8), :] = value
        own[block] = planes(value)
        extended[block] = planes(value * mine)

    for c in range(nh):
        extended[nb + (1 - served) * nh + c] = jnp.zeros((16, LANES), bf16)

    def to_partner(src_ref, dst_ref, send_sem, recv_sem):
        copy = pltpu.make_async_remote_copy(
            src_ref=src_ref, dst_ref=dst_ref, send_sem=send_sem, recv_sem=recv_sem,
            device_id={"rows": partner}, device_id_type=MESH,
        )
        copy.start()
        return copy

    def boundary_row(c):
        return jnp.broadcast_to(boundary_of[c : c + 1, :], (8, LANES))

    def send_start_halo():
        for c in range(nh):
            start_halo_send[c] = found_of(lambda s: block_of(0, s), boundary_row(c), nb)
        return to_partner(start_halo_send, start_halo_recv, halo_ssem.at[0], halo_rsem.at[0])

    def send_root_halo():
        for g in range(nh // 8):
            where = boundary_of[g * 8 : g * 8 + 8, :]
            root_halo_send[g * 8 : g * 8 + 8, :] = found_of(
                lambda s: jnp.broadcast_to(inv_root[s : s + 1, :], (8, LANES)), where, nb
            )
        return to_partner(root_halo_send, root_halo_recv, root_ssem, root_rsem)

    def gather_block(step, c):
        found = found_of(lambda s: scaled[s * 8 : s * 8 + 8, :], boundary_row(c), nb)
        halo_send[step, c] = found.astype(bf16)

    def send_halo(step):
        return to_partner(halo_send.at[step], halo_recv.at[step], halo_ssem.at[step], halo_rsem.at[step])

    def take_halo(step):
        for c in range(nh):
            if step:
                pieces = jnp.concatenate([halo_recv[step, c], jnp.zeros((8, LANES), bf16)], axis=0)
            else:
                pieces = planes(jnp.broadcast_to(root_halo_recv[c : c + 1, :], (8, LANES)) * start_halo_recv[c])
            extended[nb + served * nh + c] = pieces

    def send_returns(step):
        send, recv = (ret_send.at[step], ret_recv.at[step]) if step else (first_send, first_recv)
        for c in range(nh):
            send[c] = col_sums[table[COL_END, nb + served * nh + c]].astype(send.dtype)
        return to_partner(send, recv, ret_ssem.at[step], ret_rsem.at[step])

    def take_returns(step):
        for c in range(nh):
            returned[c] = ret_recv[step, c].astype(f32)

    def scatter_block(step, block):
        where = jnp.broadcast_to(inverse[pl.ds(served * nb + block, 1), :], (8, LANES))
        source = returned if step else first_recv
        part_send[step, block] = found_of(lambda s: source[s], where, nh)

    loads[5].wait()
    ones = jnp.concatenate([jnp.ones((8, LANES), bf16), jnp.zeros((8, LANES), bf16)], axis=0)
    products(lambda b: ones, tiles, col_sums, BY_COL)
    for side in range(2):
        for c in range(nh):
            deg_send[side, c : c + 1, :] = col_sums[table[COL_END, nb + side * nh + c], 0:1, :]
    deg_copies = exchange(
        lambda side: deg_send.at[side], lambda side: deg_recv.at[side],
        lambda side: deg_ssem.at[side], lambda side: deg_rsem.at[side],
    )
    for copy in deg_copies:
        copy.start()

    def turn(t, carry):
        turned[t] = tiles[t].T
        return carry

    lax.fori_loop(0, slots, turn, 0, unroll=16)
    products(lambda b: ones, turned, row_sums, BY_ROW)

    wait_for(gathered.at[pl.ds(0, n_probe - 1)], start_send, start_recv)

    def take_start(block, carry):
        where = pl.ds(pl.multiple_of(block * LANES, LANES), LANES)
        for g in range(n_probe):
            vec[0, pl.ds(block * 8 + g * probes_dev, probes_dev), :] = gathered[g, :, where]
        return carry

    lax.fori_loop(0, nb, take_start, 0, unroll=8)
    start_halo = send_start_halo()
    gram_begin(0, grams([(0, 0)]))
    for b in range(nb):
        inv_root[b : b + 1, :] = row_sums[table[ROW_END, b], 0:1, :] + col_sums[table[COL_END, b], 0:1, :]
    for copy in deg_copies:
        copy.wait()
    for g in range(nb // 8):
        degree = 1.0 + inv_root[g * 8 : g * 8 + 8, :]
        for side in range(2):
            degree = degree + found_of(
                lambda s: jnp.broadcast_to(deg_recv[side, s : s + 1, :], (8, LANES)),
                inverse[side * nb + g * 8 : side * nb + g * 8 + 8, :], nh,
            )
        inv_root[g * 8 : g * 8 + 8, :] = 1.0 / jnp.sqrt(degree)


    def part_copy(step, piece):
        where = pl.ds(piece * (nb // PIECES), nb // PIECES)
        return pltpu.make_async_remote_copy(
            src_ref=part_send.at[step, where], dst_ref=part_recv.at[step, where],
            send_sem=part_ssem.at[step], recv_sem=part_rsem.at[step],
            device_id={"probe": sibling}, device_id_type=MESH,
        )

    def send_parts(step):
        size = nb // PIECES
        for piece in range(PIECES):
            for block in range(piece * size, (piece + 1) * size):
                part_send[step, block] = (
                    part_send[step, block] + row_sums[table[ROW_END, block]] + mine * col_sums[table[COL_END, block]]
                )
            part_copy(step, piece).start()

    def image_of(step, source, block):
        root = root_of(block)
        return -(root * (root * block_of(source, block) + (part_send[step, block] + part_recv[step, block])))

    start_at = 0

    def q_at(j):
        return j

    def u_at(j):
        return STEPS + j

    def close(step, gram, coupling):
        shift = gram[8:]
        rest = minus(gram[:8], outer(shift))
        if coupling is not None:
            rest = minus(rest, outer(coupling))
        factor, inv_cols, next_coupling = factorise(rest)
        put_matrix(step - 1, [column + jnp.where(sub == q, 1.0, 0.0) for q, column in enumerate(shift)])
        put_matrix(STEPS + step - 1, factor)
        less = [[-column for column in product(inv_cols, shift)]]
        if coupling is not None:
            less.append([-column for column in product(inv_cols, coupling)])
        return inv_cols, less, next_coupling

    def scale_start(block, carry):
        scale_block(block, block_of(start_at, block))
        return carry

    root_halo = send_root_halo()
    lax.fori_loop(0, nb, scale_start, 0, unroll=4)
    coupling = None
    for step in range(STEPS):
        source = u_at(step) if step else start_at
        accs = [zero] * 16

        def gram_block(block):
            image = block_of(source, block)
            for q in range(8):
                accs[q] = accs[q] + image * row_of(source, block, q)
                accs[8 + q] = accs[8 + q] + image * row_of(q_at(step), block, q)

        beside = []
        if step:
            for c in range(nh):
                beside.append(functools.partial(gather_block, step, c))
                beside += [functools.partial(gram_block, 2 * c + i) for i in range(2)]
        products(lambda b: own[b], tiles, col_sums, BY_COL, beside)
        halo = send_halo(step) if step else start_halo
        returns = send_returns(step)
        if step:
            gram_begin(step, accs)
        halo.wait()
        if step == 0:
            root_halo.wait()
        take_halo(step)
        returns.wait()
        if step:
            take_returns(step)
        scatters = [functools.partial(scatter_block, step, block) for block in range(nb)]
        products(lambda b: extended[b], turned, row_sums, BY_ROW, scatters)
        send_parts(step)
        gram = gram_end(step, 16 if step else 8)
        if step:
            inv_cols, less, coupling = close(step, gram, coupling)
        else:
            _, inv_cols, _ = factorise(gram)
            less = []
        u_terms = [(columns, u_at(step - i)) for i, columns in enumerate(less)]
        if u_terms:
            mix(u_terms, u_at(step + 1))
        q_terms = [(inv_cols, source)] + [(columns, q_at(step - i)) for i, columns in enumerate(less)]
        mix(q_terms, q_at(step + 1))
        wait_for(part_recv.at[step], part_ssem.at[step], part_rsem.at[step])

        def next_image(block, carry):
            image = image_of(step, source, block)
            value = inv_cols[0] * spread(image, 0)
            for q in range(1, 8):
                value = value + inv_cols[q] * spread(image, q)
            if u_terms:
                value = value + block_of(u_at(step + 1), block)
            put_block(u_at(step + 1), block, value)
            if step + 1 < STEPS:
                scale_block(block, value)
            return carry

        lax.fori_loop(0, nb, next_image, 0, unroll=4)

    gram_begin(STEPS, grams([(u_at(STEPS), u_at(STEPS)), (u_at(STEPS), q_at(STEPS))]))
    gram = gram_end(STEPS, 16)
    inv_cols, less, _ = close(STEPS, gram, coupling)
    terms = [(inv_cols, u_at(STEPS))] + [(columns, q_at(STEPS - i)) for i, columns in enumerate(less)]
    for i, (columns, _) in enumerate(terms):
        for q in range(8):
            spare[i * 64 + q * 8 : i * 64 + q * 8 + 8, :] = columns[q]
    for p in range(probes_dev):
        total = jnp.zeros((nb, LANES), f32)
        for i, (_, k) in enumerate(terms):
            for q in range(8):
                weight = spare[pl.ds(i * 64 + q * 8 + my_probe * probes_dev + p, 1), :]
                total = total + jnp.broadcast_to(weight, (nb, LANES)) * vec[k, pl.ds(q, nb, stride=8), :]
        basis_ref[p] = total


def in_hbm(value):
    return pltpu.with_memory_space_constraint(value, pltpu.HBM)


def local(start_block, blocks, block_rows, block_cols, counts, boundary):
    n_rows, n_probe = lax.axis_size("rows"), lax.axis_size("probe")
    probes_dev, rows_dev = start_block.shape
    slots = blocks.shape[0]
    nb = rows_dev // LANES
    nh = nb // 2
    f32, bf16 = jnp.float32, jnp.bfloat16
    vmem = pl.BlockSpec(memory_space=pltpu.VMEM)
    dma = pltpu.SemaphoreType.DMA
    basis, coef = pl.pallas_call(
        functools.partial(kernel, n_rows, n_probe, rows_dev * n_rows),
        out_shape=(
            jax.ShapeDtypeStruct((probes_dev, nb, LANES), f32),
            jax.ShapeDtypeStruct((2 * STEPS, 8, LANES), f32),
        ),
        in_specs=[pl.BlockSpec(memory_space=pltpu.HBM)] * 6,
        out_specs=(vmem, vmem),
        scratch_shapes=[
            pltpu.VMEM(start_block.shape, f32),
            pltpu.VMEM(blocks.shape, bf16),
            pltpu.VMEM(blocks.shape, bf16),
            pltpu.VMEM((1, slots), jnp.int32),
            pltpu.VMEM((1, slots), jnp.int32),
            pltpu.SMEM(counts.shape, jnp.int32),
            pltpu.VMEM(boundary.shape, jnp.int32),
            pltpu.VMEM((n_probe, probes_dev, rows_dev), f32),
            pltpu.VMEM((2 * STEPS + 1, nb * 8, LANES), f32),
            pltpu.VMEM((3 * 64, LANES), f32),
            pltpu.VMEM((nb * 8, LANES), f32),
            pltpu.VMEM((nb, LANES), f32),
            pltpu.VMEM((2 * nb, LANES), jnp.int32),
            pltpu.VMEM((8, LANES), jnp.int32),
            pltpu.SMEM((8, LANES), jnp.int32),
            pltpu.VMEM((nh, LANES), jnp.int32),
            pltpu.VMEM((nb, 16, LANES), bf16),
            pltpu.VMEM((2 * nb, 16, LANES), bf16),
            pltpu.VMEM((nh, 8, LANES), f32),
            pltpu.VMEM((nh, 8, LANES), f32),
            pltpu.VMEM((nh, LANES), f32),
            pltpu.VMEM((nh, LANES), f32),
            pltpu.VMEM((STEPS, nh, 8, LANES), bf16),
            pltpu.VMEM((STEPS, nh, 8, LANES), bf16),
            pltpu.VMEM((nh, 8, LANES), f32),
            pltpu.VMEM((nh, 8, LANES), f32),
            pltpu.VMEM((STEPS, nh, 8, LANES), bf16),
            pltpu.VMEM((STEPS, nh, 8, LANES), bf16),
            pltpu.VMEM((nh, 8, LANES), f32),
            pltpu.VMEM((2, nh, LANES), f32),
            pltpu.VMEM((2, nh, LANES), f32),
            pltpu.VMEM((STEPS, nb, 8, LANES), f32),
            pltpu.VMEM((STEPS, nb, 8, LANES), f32),
            pltpu.VMEM((slots + 1, 8, LANES), f32),
            pltpu.VMEM((slots + 1, 8, LANES), f32),
            pltpu.VMEM((STEPS + 1, 8, LANES), f32),
            pltpu.VMEM((STEPS + 1, n_rows, 8, LANES), f32),
            dma((6,)),
            dma,
            dma,
            dma,
            dma,
            dma,
            dma((STEPS,)),
            dma((STEPS,)),
            dma((STEPS,)),
            dma((STEPS,)),
            dma((STEPS,)),
            dma((STEPS,)),
            dma((2,)),
            dma((2,)),
            dma((STEPS + 1,)),
            dma((STEPS + 1,)),
        ],
        compiler_params=pltpu.CompilerParams(
            collective_id=0, has_side_effects=True, vmem_limit_bytes=VMEM_BYTES
        ),
        name="lanczos",
    )(
        in_hbm(start_block), in_hbm(blocks), in_hbm(block_rows.reshape(1, slots)),
        in_hbm(block_cols.reshape(1, slots)), counts, in_hbm(boundary),
    )
    return basis.reshape(probes_dev, rows_dev), coef[:STEPS, :, :8], coef[STEPS:, :, :8]


def solution(mesh):
    in_specs = (
        P("probe", "rows"),
        P("rows", None, None),
        P("rows"),
        P("rows"),
        P("rows"),
        P(None, "rows"),
    )
    out_specs = (P("probe", "rows"), P(), P())
    return jax.shard_map(local, mesh=mesh, in_specs=in_specs, out_specs=out_specs, check_vma=False)
```
